32 devices in a mesh: row: 4 (over z), col: 8 (over y, x, core).
Axes of the slice: x: 2, y: 2, z: 4, core: 2. Of those that a mesh axis runs over, the one named last changes fastest.
Arguments:
- points_rhs: bfloat16 [262144, 16], P(('row', 'col')), may hold values from -6 to 6
- leaf_basis: bfloat16 [1024, 256, 64], P(('row', 'col')), may hold values from -0.375 to 0.375
- near_src: int32 [1024, 2], P(('row', 'col')), may hold values from -1 to 1023, as said below
- near_blocks: bfloat16 [1024, 2, 256, 256], P(('row', 'col')), may hold values from -0.25 to 0.25
- transfer_first: bfloat16 [1024, 64, 64], P(('row', 'col')), may hold values from -0.5 to 0.5
- transfer_second: bfloat16 [512, 64, 64], P(('row', 'col')), may hold values from -0.5 to 0.5
- transfer_third: bfloat16 [256, 64, 64], P(('row', 'col')), may hold values from -0.5 to 0.5
- far_zero: int32 [1024, 8], P(('row', 'col')), may hold values from -1 to 1023, as said below
- far_one: int32 [512, 8], P(('row', 'col')), may hold values from -1 to 511, as said below
- far_two: int32 [256, 8], P(('row', 'col')), may hold values from -1 to 255, as said below
- far_three: int32 [128, 8], P(('row', 'col')), may hold values from -1 to 127, as said below
- couple_zero: bfloat16 [1024, 8, 64, 64], P(('row', 'col')), may hold values from -0.25 to 0.25
- couple_one: bfloat16 [512, 8, 64, 64], P(('row', 'col')), may hold values from -0.25 to 0.25
- couple_two: bfloat16 [256, 8, 64, 64], P(('row', 'col')), may hold values from -0.25 to 0.25
- couple_three: bfloat16 [128, 8, 64, 64], P(('row', 'col')), may hold values from -0.25 to 0.25
Outputs:
- product: bfloat16 [262144, 16], P(('row', 'col'))
The draws below stay inside these ranges and needn't reach their ends.
Inputs may be any that keep to these rules, and one draw needn't show every extreme that they name: `near_src`: each entry is -1 or a leaf whose index differs from its row's by at most 2; -1 only where that leaf would lie outside the grid. `far_zero`: each row has 7 or 8 live entries, first in the row; a live entry of leaf i lies in the same aligned block of 256 leaves as i. `far_one`: each row has 7 or 8 live entries, first in the row; a live entry of cluster i lies in the same aligned block of 128 clusters as i. `far_two`: each row has 7 or 8 live entries, first in the row; a live entry of cluster i lies in the same aligned block of 64 clusters as i. `far_three`: each row has 7 or 8 live entries, first in the row; live entries may name any cluster of the level.
All inputs are finite; a program needn't handle non-finite values.
Results may differ from the reference program's by a relative error of at most 0.0044.
Values may be sent and summed in bfloat16 or wider, within the bound.
No kernel may reach another device: no remote copies, remote signals or barrier semaphores. Data moves between devices by JAX's collectives and lax.ppermute only.
A program may use at most 128 MiB of HBM per device.

```python
import jax
import jax.numpy as jnp
from jax import lax

LEAF = 256
RANK = 64
NRHS = 16
SLOTS = 8
NEAR = 2
LEAF_DEV = 32
LEAVES = 1024
NPTS = 262144
GROUP = 256


def far_list(key, level_index):
    total_rows = LEAVES // 2 ** level_index
    group_size = GROUP // 2 ** level_index if level_index < 3 else total_rows
    first_key, second_key = jax.random.split(jax.random.fold_in(key, 100 + level_index))
    row_ids = jnp.arange(total_rows, dtype=jnp.int32)
    group_start = row_ids // group_size * group_size
    sources = group_start[:, None] + jax.random.randint(first_key, (total_rows, SLOTS), 0, group_size, dtype=jnp.int32)
    live_count = jax.random.randint(second_key, (total_rows, 1), SLOTS - 1, SLOTS + 1, dtype=jnp.int32)
    is_live = jnp.arange(SLOTS, dtype=jnp.int32)[None, :] < live_count
    return jnp.where(is_live, sources, -1).astype(jnp.int32)


def draw_near_src(key, part):
    row_ids = jnp.arange(LEAVES, dtype=jnp.int32)
    offsets = jax.random.randint(jax.random.fold_in(key, 7), (LEAVES, NEAR), -2, 3, dtype=jnp.int32)
    sources = row_ids[:, None] + offsets
    inside = (sources >= 0) & (sources < LEAVES)
    return jnp.where(inside, sources, -1).astype(jnp.int32)


def draw_far_zero(key, part):
    return far_list(key, 0)


def draw_far_one(key, part):
    return far_list(key, 1)


def draw_far_two(key, part):
    return far_list(key, 2)


def draw_far_three(key, part):
    return far_list(key, 3)


def block_scale(key, dims, cuts, low, high):
    level, own = 1.0, jax.random.fold_in(key, 6)
    for position, shards_of in cuts:
        draws = jnp.exp(jax.random.uniform(jax.random.fold_in(own, position), (shards_of,), jnp.float32, low / len(cuts), high / len(cuts)))
        level = level * jnp.repeat(draws, dims[position] // shards_of).reshape([-1 if axis == position else 1 for axis in range(len(dims))])
    return level


def scatter_about(rng, extent, scale, bound, cuts=(), kind=jnp.bfloat16):
    drawn = jax.random.normal(rng, extent, jnp.float32) * scale
    if len(cuts) > 0:
        drawn = block_scale(rng, extent, cuts, -0.22, 0.18) * drawn
    return jnp.clip(drawn, min=-bound, max=bound).astype(kind)


def setup_inputs(seed: int = 0) -> dict:
    streams_of = jax.random.split(jax.random.key(seed), 16)
    points_rhs = scatter_about(streams_of[0], (NPTS, NRHS), 1.0, 6.0, ((0, 32),))
    leaf_basis = scatter_about(streams_of[1], (LEAVES, LEAF, RANK), LEAF ** -0.5, 0.375, ((0, 32),))
    near_src = draw_near_src(jax.random.fold_in(streams_of[15], 71), 0)
    near_blocks = scatter_about(streams_of[3], (LEAVES, NEAR, LEAF, LEAF), (LEAF * NEAR) ** -0.5, 0.25, ((0, 32),))
    transfer_first = scatter_about(streams_of[4], (LEAVES, RANK, RANK), (2 * RANK) ** -0.5, 0.5, ((0, 32),))
    transfer_second = scatter_about(streams_of[5], (LEAVES // 2, RANK, RANK), (2 * RANK) ** -0.5, 0.5, ((0, 32),))
    transfer_third = scatter_about(streams_of[6], (LEAVES // 4, RANK, RANK), (2 * RANK) ** -0.5, 0.5, ((0, 32),))
    far_zero = draw_far_zero(jax.random.fold_in(streams_of[15], 71), 0)
    far_one = draw_far_one(jax.random.fold_in(streams_of[15], 71), 0)
    far_two = draw_far_two(jax.random.fold_in(streams_of[15], 71), 0)
    far_three = draw_far_three(jax.random.fold_in(streams_of[15], 71), 0)
    couple_zero = scatter_about(streams_of[11], (LEAVES, SLOTS, RANK, RANK), (RANK * SLOTS) ** -0.5, 0.25, ((0, 32),))
    couple_one = scatter_about(streams_of[12], (LEAVES // 2, SLOTS, RANK, RANK), (RANK * SLOTS) ** -0.5, 0.25, ((0, 32),))
    couple_two = scatter_about(streams_of[13], (LEAVES // 4, SLOTS, RANK, RANK), (RANK * SLOTS) ** -0.5, 0.25, ((0, 32),))
    couple_three = scatter_about(streams_of[14], (LEAVES // 8, SLOTS, RANK, RANK), (RANK * SLOTS) ** -0.5, 0.25, ((0, 32),))
    return dict(points_rhs=points_rhs, leaf_basis=leaf_basis, near_src=near_src, near_blocks=near_blocks, transfer_first=transfer_first, transfer_second=transfer_second, transfer_third=transfer_third, far_zero=far_zero, far_one=far_one, far_two=far_two, far_three=far_three, couple_zero=couple_zero, couple_one=couple_one, couple_two=couple_two, couple_three=couple_three)


TOP_LEVEL = lax.Precision.HIGHEST


def gather_active(table, sources):
    is_live = (sources >= 0).astype(jnp.float32)
    selected_rows = jnp.take(table, jnp.clip(sources, 0, table.shape[0] - 1).astype(jnp.int32), axis=0).astype(jnp.float32)
    return selected_rows * is_live[:, :, None, None]


def reference(points_rhs, leaf_basis, near_src, near_blocks, transfer_first, transfer_second, transfer_third, far_zero, far_one, far_two, far_three, couple_zero, couple_one, couple_two, couple_three):
    leaf_x = points_rhs.reshape(LEAVES, LEAF, NRHS)
    basis_f = leaf_basis.astype(jnp.float32)
    skel_zero = jnp.einsum("lpa,lpr->lar", basis_f, leaf_x.astype(jnp.float32), precision=TOP_LEVEL).astype(jnp.bfloat16)
    skeletons = [skel_zero]
    transfers = [transfer_first, transfer_second, transfer_third]
    for transfer in transfers:
        child_skel = skeletons[-1]
        lifted = jnp.einsum("cab,car->cbr", transfer.astype(jnp.float32), child_skel.astype(jnp.float32), precision=TOP_LEVEL)
        lifted = lifted.reshape(lifted.shape[0] // 2, 2, RANK, NRHS).sum(axis=1)
        skeletons.append(lifted.astype(jnp.bfloat16))
    lists = [far_zero, far_one, far_two, far_three]
    coupling_blocks = [couple_zero, couple_one, couple_two, couple_three]
    coupled_field = []
    for level_index in range(4):
        selected_rows = gather_active(skeletons[level_index], lists[level_index])
        coupled_field.append(jnp.einsum("enyd,endc->eyc", coupling_blocks[level_index].astype(jnp.float32), selected_rows, precision=TOP_LEVEL))
    downward_field = coupled_field[3]
    for level_index in (3, 2, 1):
        spread = jnp.repeat(downward_field, 2, axis=0)
        downward_field = coupled_field[level_index - 1] + jnp.einsum("cab,cbr->car", transfers[level_index - 1].astype(jnp.float32), spread, precision=TOP_LEVEL)
    far_out = jnp.einsum("lpa,lar->lpr", basis_f, downward_field, precision=TOP_LEVEL)

    def near_piece(pair):
        blocks, sources = pair
        selected_rows = gather_active(leaf_x, sources)
        return jnp.einsum("iknm,ikmr->inr", blocks.astype(jnp.float32), selected_rows, precision=TOP_LEVEL)

    pieces = LEAVES // LEAF_DEV
    near_out = lax.map(near_piece, (near_blocks.reshape(pieces, LEAF_DEV, NEAR, LEAF, LEAF), near_src.reshape(pieces, LEAF_DEV, NEAR)))
    near_out = near_out.reshape(LEAVES, LEAF, NRHS)
    return (far_out + near_out).reshape(NPTS, NRHS).astype(jnp.bfloat16)
```

```python
import functools

import jax
import jax.numpy as jnp
from jax import lax
from jax.experimental import pallas as pl
from jax.experimental.pallas import tpu as pltpu
from jax.sharding import PartitionSpec as P

SLOTS = 8
HALO = 2
STEPS = 8


NT = (((1,), (1,)), ((), ()))
NN = (((1,), (0,)), ((), ()))
TN = (((0,), (0,)), ((), ()))

VMEM = pl.BlockSpec(memory_space=pltpu.VMEM)
SMEM = pl.BlockSpec(memory_space=pltpu.SMEM)


def dot(a, b, dims):
    return lax.dot_general(a, b, dims, preferred_element_type=jnp.float32)


def low_half(shape):
    return lax.broadcasted_iota(jnp.int32, shape, len(shape) - 1) < shape[-1] // 2


def upward_kernel(n0, leaf, x_ref, basis_ref, e1_ref, e2_ref, e3_ref, skel_ref, top_ref, head_ref, tail_ref):
    head_ref[...] = x_ref[:, : HALO * leaf]
    tail_ref[...] = x_ref[:, (n0 - HALO) * leaf :]
    nrhs = x_ref.shape[0]
    low = low_half((nrhs, 128))
    level = []
    for p in range(n0 // 2):
        xs = jnp.concatenate([x_ref[:, (2 * p + h) * leaf : (2 * p + h + 1) * leaf] for h in range(2)], axis=0)
        both = dot(xs, basis_ref[p], NT)
        level.append(jnp.where(low, both[:nrhs], both[nrhs:]).astype(jnp.bfloat16))
        skel_ref[p] = level[p]
    base = n0 // 2
    for e_ref, out_ref in ((e1_ref, skel_ref), (e2_ref, skel_ref), (e3_ref, top_ref)):
        parents = [dot(v, e_ref[p], NN) for p, v in enumerate(level)]
        level = [
            jnp.concatenate([parents[2 * q], parents[2 * q + 1]], axis=1).astype(jnp.bfloat16)
            for q in range(len(parents) // 2)
        ]
        if out_ref is top_ref:
            base = 0
        for q, v in enumerate(level):
            out_ref[base + q] = v
        base += len(level)


def local_kernel(
    n0, leaf, cols, rows, near_src_ref, left_ref, right_ref, x_ref, blocks_ref,
    f0_ref, f1_ref, f2_ref, f3_ref, s0_ref, s1_ref, s2_ref, s3_ref,
    near_ref, i0_ref, i1_ref, i2_ref, i3_ref, c0_ref, c1_ref, c2_ref, c3_ref, xp_ref,
):
    step = pl.program_id(0)
    row, col = lax.axis_index("row"), lax.axis_index("col")
    zero_block = n0 + 2 * HALO
    pairs = (n0 // 2 + n0 // 4 + n0 // 8) + rows * (n0 // 16)

    @pl.when(step == 0)
    def _():
        xp_ref[:, : HALO * leaf] = left_ref[...]
        xp_ref[:, HALO * leaf : (HALO + n0) * leaf] = x_ref[...]
        xp_ref[:, (HALO + n0) * leaf : zero_block * leaf] = right_ref[...]
        xp_ref[:, zero_block * leaf :] = jnp.zeros((x_ref.shape[0], leaf), jnp.bfloat16)

        def place(f, slot_axis, per, first_pair, kz):
            dev = f // per
            pos = f % per
            k = (dev % cols) ^ col
            if kz:
                first_pair = first_pair + ((dev // cols) ^ row) * (per // 2)
            block = (k % 2) * (cols // 2) + k // 2
            spot = (block * pairs + first_pair) * 2 + pos
            slot = lax.broadcasted_iota(jnp.int32, f.shape, slot_axis)
            spot = spot ^ (slot % 2)
            return jnp.where(f >= 0, spot, cols * pairs * 2)

        i0_ref[...] = place(f0_ref[...], 0, n0, 0, False)
        i1_ref[...] = place(f1_ref[...], 0, n0 // 2, n0 // 2, False)
        i2_ref[...] = place(f2_ref[...], 1, n0 // 4, n0 // 2 + n0 // 4, False)
        i3_ref[...] = place(f3_ref[...], 1, n0 // 8, n0 // 2 + n0 // 4 + n0 // 8, True)

    count = blocks_ref.shape[0]
    first_leaf = (row * cols + col) * n0
    for j in range(count):
        acc = None
        for s in range(2):
            src = near_src_ref[s, step * count + j]
            at = jnp.where(src >= 0, src - first_leaf + HALO, zero_block)
            xs = xp_ref[:, pl.ds(pl.multiple_of(at * leaf, leaf), leaf)]
            part = dot(xs, blocks_ref[j, s], NT)
            acc = part if acc is None else acc + part
        near_ref[:, j * leaf : (j + 1) * leaf] = acc

    def repack(s_ref, c_ref):
        for c in range(s_ref.shape[0]):
            for q in range(SLOTS // 2):
                c_ref[c, :, q * 128 : (q + 1) * 128] = jnp.concatenate(
                    [s_ref[c, 2 * q], s_ref[c, 2 * q + 1]], axis=1
                )

    repack(s0_ref, c0_ref)
    repack(s1_ref, c1_ref)
    repack(s2_ref, c2_ref)

    @pl.when(step % 2 == 0)
    def _():
        repack(s3_ref, c3_ref)


def product_kernel(
    n0, leaf, i0_ref, i1_ref, i2_ref, i3_ref, a_ref, b_ref, c0_ref, c1_ref, c2_ref, c3_ref,
    e1_ref, e2_ref, e3_ref, basis_ref, near_ref, out_ref, table_ref, field_ref,
):
    half = a_ref.shape[0]
    nrhs = out_ref.shape[0]
    low = low_half((nrhs, 128))

    def spread(p, carry):
        for h, ref in enumerate((a_ref, b_ref)):
            v = ref[p]
            table_ref[(h * half + p) * 2] = v
            table_ref[(h * half + p) * 2 + 1] = jnp.concatenate([v[:, 64:], v[:, :64]], axis=1)
        return carry

    lax.fori_loop(0, half, spread, 0, unroll=8)
    table_ref[4 * half] = jnp.zeros((nrhs, 128), jnp.bfloat16)
    table_ref[4 * half + 1] = jnp.zeros((nrhs, 128), jnp.bfloat16)

    def couple(c_ref, spot, i):
        xs = [
            jnp.where(low, table_ref[spot(2 * q, i)], table_ref[spot(2 * q + 1, i)])
            for q in range(SLOTS // 2)
        ]
        return dot(c_ref[i], jnp.concatenate(xs, axis=1), NT)

    def by_slot(ref):
        return lambda k, i: ref[k, i]

    def by_row(ref):
        return lambda k, i: ref[i, k]

    down = [couple(c3_ref, by_row(i3_ref), i) for i in range(n0 // 8)]
    for e_ref, c_ref, spot in (
        (e3_ref, c2_ref, by_row(i2_ref)),
        (e2_ref, c1_ref, by_slot(i1_ref)),
    ):
        below = []
        for p, d in enumerate(down):
            pair = dot(e_ref[p], d.astype(jnp.bfloat16), NN)
            for h in range(2):
                below.append(couple(c_ref, spot, 2 * p + h) + pair[h * 64 : (h + 1) * 64])
        down = below
    for p, d in enumerate(down):
        field_ref[p] = d.astype(jnp.bfloat16)

    def leaves(p):
        pair = dot(e1_ref[p], field_ref[p], NN)
        for h in range(2):
            i = 2 * p + h
            d = couple(c0_ref, by_slot(i0_ref), i) + pair[h * 64 : (h + 1) * 64]
            far = dot(d.astype(jnp.bfloat16), basis_ref[p, h * 64 : (h + 1) * 64], TN)
            at = pl.ds(pl.multiple_of(i * leaf, leaf), leaf)
            out_ref[:, at] = (far + near_ref[:, at]).astype(jnp.bfloat16)

    for p in range(n0 // 2):
        leaves(p)


def shards(
    points_rhs, leaf_basis, near_src, near_blocks, transfer_first, transfer_second, transfer_third,
    far_zero, far_one, far_two, far_three, couple_zero, couple_one, couple_two, couple_three,
):
    bf = jnp.bfloat16
    n0, leaf, rank = leaf_basis.shape
    nrhs = points_rhs.shape[1]
    rows, cols = lax.axis_size("row"), lax.axis_size("col")
    x = points_rhs.T
    basis = leaf_basis.transpose(0, 2, 1).reshape(n0 // 2, 2 * rank, leaf)
    e1, e2, e3 = (
        e.reshape(e.shape[0] // 2, 2 * rank, rank) for e in (transfer_first, transfer_second, transfer_third)
    )
    own_pairs = n0 // 2 + n0 // 4 + n0 // 8
    top_pairs = n0 // 16
    skel, top, head, tail = pl.pallas_call(
        functools.partial(upward_kernel, n0, leaf),
        out_shape=[
            jax.ShapeDtypeStruct((own_pairs, nrhs, 2 * rank), bf),
            jax.ShapeDtypeStruct((top_pairs, nrhs, 2 * rank), bf),
            jax.ShapeDtypeStruct((nrhs, HALO * leaf), bf),
            jax.ShapeDtypeStruct((nrhs, HALO * leaf), bf),
        ],
        in_specs=[VMEM] * 5,
        out_specs=[VMEM] * 4,
        compiler_params=pltpu.CompilerParams(vmem_limit_bytes=12 << 20),
        cost_estimate=pl.CostEstimate(flops=2 * n0 * rank * leaf * nrhs * 2, bytes_accessed=2 << 20, transcendentals=0),
        name="upward",
    )(x, basis, e1, e2, e3)

    total = rows * cols
    line = ("row", "col")
    left = lax.ppermute(tail, line, [(i, i + 1) for i in range(total - 1)])
    right = lax.ppermute(head, line, [(i + 1, i) for i in range(total - 1)])

    def swap(v, axis, size, k):
        return lax.ppermute(v, axis, [(i, i ^ k) for i in range(size)])

    tops = [None] * rows
    tops[0] = top
    for k in reversed(range(1, rows)):
        tops[k] = swap(top, "row", rows, k)
    mine = jnp.concatenate([skel] + tops, axis=0)
    parts = [None] * (cols // 2)
    parts[0] = mine
    for k in reversed(range(1, cols // 2)):
        parts[k] = swap(mine, "col", cols, 2 * k)

    pairs = mine.shape[0]
    n1, n2, n3 = n0 // 2, n0 // 4, n0 // 8

    def lead(shape, index=lambda i: i):
        return pl.BlockSpec(shape, lambda i: (index(i),) + (0,) * (len(shape) - 1))

    def fixed(shape):
        return pl.BlockSpec(shape, lambda i: (0,) * len(shape))

    def wide(n):
        return jax.ShapeDtypeStruct((n, rank, SLOTS * rank), bf)

    lists = (far_zero.T, far_one.T, far_two, far_three)
    per = [n // STEPS for n in (n0, n1, n2)]
    near, i0, i1, i2, i3, c0, c1, c2, c3 = pl.pallas_call(
        functools.partial(local_kernel, n0, leaf, cols, rows),
        grid=(STEPS,),
        out_shape=[jax.ShapeDtypeStruct((nrhs, n0 * leaf), jnp.float32)]
        + [jax.ShapeDtypeStruct(f.shape, jnp.int32) for f in lists]
        + [wide(n) for n in (n0, n1, n2, n3)],
        in_specs=[
            SMEM,
            fixed((nrhs, HALO * leaf)),
            fixed((nrhs, HALO * leaf)),
            fixed((nrhs, n0 * leaf)),
            lead((per[0], 2, leaf, leaf)),
        ]
        + [fixed(f.shape) for f in lists]
        + [lead((n, SLOTS, rank, rank)) for n in per]
        + [lead((1, SLOTS, rank, rank), lambda i: i // 2)],
        out_specs=[pl.BlockSpec((nrhs, per[0] * leaf), lambda i: (0, i))]
        + [fixed(f.shape) for f in lists]
        + [lead((n, rank, SLOTS * rank)) for n in per]
        + [lead((1, rank, SLOTS * rank), lambda i: i // 2)],
        scratch_shapes=[pltpu.VMEM((nrhs, (n0 + 2 * HALO + 1) * leaf), bf)],
        compiler_params=pltpu.CompilerParams(
            dimension_semantics=("arbitrary",), vmem_limit_bytes=24 << 20
        ),
        cost_estimate=pl.CostEstimate(flops=40 * n0 * leaf * leaf * nrhs, bytes_accessed=20 << 20, transcendentals=0),
        name="local",
    )(near_src.T, left, right, x, near_blocks, *lists, couple_zero, couple_one, couple_two, couple_three)

    ours = jnp.concatenate(parts, axis=0)
    theirs = swap(ours, "col", cols, 1)
    out = pl.pallas_call(
        functools.partial(product_kernel, n0, leaf),
        out_shape=jax.ShapeDtypeStruct((nrhs, n0 * leaf), bf),
        in_specs=[SMEM] * 4 + [VMEM] * 11,
        out_specs=VMEM,
        scratch_shapes=[
            pltpu.VMEM((2 * cols * pairs + 2, nrhs, 2 * rank), bf),
            pltpu.VMEM((n1, rank, nrhs), bf),
        ],
        compiler_params=pltpu.CompilerParams(vmem_limit_bytes=32 << 20),
        cost_estimate=pl.CostEstimate(flops=2 * n0 * leaf * leaf * nrhs, bytes_accessed=8 << 20, transcendentals=0),
        name="product",
    )(i0, i1, i2, i3, ours, theirs, c0, c1, c2, c3, e1, e2, e3, basis, near)
    return out.T


def solution(mesh):
    whole = P(("row", "col"))
    return jax.shard_map(
        shards,
        mesh=mesh,
        in_specs=(whole,) * 15,
        out_specs=whole,
        check_vma=False,
    )
```

```python
import functools

import jax
import jax.numpy as jnp
from jax import lax
from jax.experimental import pallas as pl
from jax.experimental.pallas import tpu as pltpu
from jax.sharding import PartitionSpec as P

SLOTS = 8
HALO = 2
STEPS = 8
CHUNKS = 4


NT = (((1,), (1,)), ((), ()))
NN = (((1,), (0,)), ((), ()))
TN = (((0,), (0,)), ((), ()))

VMEM = pl.BlockSpec(memory_space=pltpu.VMEM)
SMEM = pl.BlockSpec(memory_space=pltpu.SMEM)
HBM = pl.BlockSpec(memory_space=pltpu.HBM)
ANY = pl.BlockSpec(memory_space=pl.ANY)


def in_hbm(v):
    return pltpu.with_memory_space_constraint(v, pltpu.HBM)


def dot(a, b, dims):
    return lax.dot_general(a, b, dims, preferred_element_type=jnp.float32)


def low_half(shape):
    return lax.broadcasted_iota(jnp.int32, shape, len(shape) - 1) < shape[-1] // 2


def copies(pairs, sems):
    return [pltpu.make_async_copy(src, dst, sems.at[i]) for i, (src, dst) in enumerate(pairs)]


def edge_blocks(ref, x_ref, at, width, first):
    for b in range(width // 128):
        ref[first + b] = x_ref[:, at + b * 128 : at + (b + 1) * 128]


def upward_kernel(
    n0, leaf, x_hbm, basis_hbm, e1_hbm, e2_hbm, e3_hbm, skel_ref, near_row_ref, far_row_ref, chip_ref, core_ref,
    x_ref, basis_ref, e1_ref, e2_ref, e3_ref, sems, basis_sems,
):
    chunk = n0 // 2 // CHUNKS
    top = n0 // 16
    width = HALO * leaf
    fetch = copies([(x_hbm, x_ref), (e1_hbm, e1_ref), (e2_hbm, e2_ref), (e3_hbm, e3_ref)], sems)
    spans = [pl.ds(c * chunk, chunk) for c in range(CHUNKS)]
    fetch_basis = copies([(basis_hbm.at[s], basis_ref.at[s]) for s in spans], basis_sems)
    fetch[0].start()
    for c in fetch_basis:
        c.start()
    for c in fetch[1:]:
        c.start()
    fetch[0].wait()

    def edges(even, head_to, tail_to):
        @pl.when(even)
        def _():
            edge_blocks(head_to[0], x_ref, 0, width, head_to[1])
            edge_blocks(tail_to[0], x_ref, n0 * leaf - width, width, tail_to[1])

        @pl.when(jnp.logical_not(even))
        def _():
            edge_blocks(tail_to[0], x_ref, 0, width, tail_to[1])
            edge_blocks(head_to[0], x_ref, n0 * leaf - width, width, head_to[1])

    edges(lax.axis_index("row") % 2 == 0, (far_row_ref, top), (near_row_ref, top))
    edges(lax.axis_index("col") % 2 == 0, (chip_ref, 0), (core_ref, 0))
    nrhs = x_ref.shape[0]
    low = low_half((nrhs, 128))
    level = []
    for p in range(n0 // 2):
        if p % chunk == 0:
            fetch_basis[p // chunk].wait()
        xs = jnp.concatenate([x_ref[:, (2 * p + h) * leaf : (2 * p + h + 1) * leaf] for h in range(2)], axis=0)
        both = dot(xs, basis_ref[p], NT)
        level.append(jnp.where(low, both[:nrhs], both[nrhs:]).astype(jnp.bfloat16))
        skel_ref[p] = level[p]
    base = n0 // 2
    for step, e_ref in enumerate((e1_ref, e2_ref, e3_ref)):
        fetch[1 + step].wait()
        parents = [dot(v, e_ref[p], NN) for p, v in enumerate(level)]
        level = [
            jnp.concatenate([parents[2 * q], parents[2 * q + 1]], axis=1).astype(jnp.bfloat16)
            for q in range(len(parents) // 2)
        ]
        for q, v in enumerate(level):
            if step < 2:
                skel_ref[base + q] = v
            else:
                near_row_ref[q] = v
                far_row_ref[q] = v
        base += len(level)


def pack_kernel(rows, cols, top, skel_ref, chip_ref, after_ref, own_ref, *refs):
    del after_ref
    own, width = skel_ref.shape[0], chip_ref.shape[0]
    tops, mine_ref = (own_ref, *refs[: rows - 1]), refs[rows - 1]
    mine_ref[:own] = skel_ref[...]
    for k in range(rows):
        mine_ref[own + k * top : own + (k + 1) * top] = tops[k][:top]
    base = own + rows * top
    mine_ref[base : base + width] = chip_ref[...]
    row, col = lax.axis_index("row"), lax.axis_index("col")
    odd = row % 2
    from_near = (col == cols - 1) == (odd == 1)
    partner = jnp.where(from_near, 1, row ^ (row + 2 * odd - 1))
    for m in range(1, rows.bit_length()):
        k = 2**m - 1
        if k >= rows:
            break

        @pl.when((partner == k) | (k == 1))
        def _(k=k):
            mine_ref[base + width :] = tops[k][top:]


def fold_kernel(
    n0, cols, rows, f0_hbm, f1_hbm, f2_hbm, f3_hbm, s0_hbm, s1_hbm, s2_hbm, s3_hbm,
    i0_ref, i1_ref, i2_ref, i3_ref, c0_ref, c1_ref, c2_ref, c3_ref,
    f0_ref, f1_ref, f2_ref, f3_ref, s0_ref, s1_ref, s2_ref, s3_ref, sems, block_sems,
):
    row, col = lax.axis_index("row"), lax.axis_index("col")
    pairs = (n0 // 2 + n0 // 4 + n0 // 8) + rows * (n0 // 16)
    lists = copies([(f0_hbm, f0_ref), (f1_hbm, f1_ref), (f2_hbm, f2_ref), (f3_hbm, f3_ref)], sems)
    streams = ((s0_hbm, s0_ref), (s1_hbm, s1_ref), (s2_hbm, s2_ref), (s3_hbm, s3_ref))

    def chunk(step):
        out = []
        for n, (src, dst) in enumerate(streams):
            size = src.shape[0] // CHUNKS
            span = pl.ds(step * size, size)
            out.append(pltpu.make_async_copy(src.at[span], dst.at[span], block_sems.at[step, n]))
        return out

    for c in lists:
        c.start()
    for step in range(CHUNKS):
        for c in chunk(step):
            c.start()
    for c in lists:
        c.wait()

    def place(f, slot_axis, per, first_pair, kz):
        dev = f // per
        pos = f % per
        k = (dev % cols) ^ col
        if kz:
            first_pair = first_pair + ((dev // cols) ^ row) * (per // 2)
        block = (k % 2) * (cols // 2) + k // 2
        spot = (block * pairs + first_pair) * 2 + pos
        slot = lax.broadcasted_iota(jnp.int32, f.shape, slot_axis)
        spot = spot ^ (slot % 2)
        return jnp.where(f >= 0, spot, cols * pairs * 2)

    i0_ref[...] = place(f0_ref[...], 0, n0, 0, False)
    i1_ref[...] = place(f1_ref[...], 0, n0 // 2, n0 // 2, False)
    i2_ref[...] = place(f2_ref[...], 1, n0 // 4, n0 // 2 + n0 // 4, False)
    i3_ref[...] = place(f3_ref[...], 1, n0 // 8, n0 // 2 + n0 // 4 + n0 // 8, True)

    @pl.loop(0, CHUNKS)
    def _(step):
        for c in chunk(step):
            c.wait()
        for s_ref, c_ref in ((s0_ref, c0_ref), (s1_ref, c1_ref), (s2_ref, c2_ref), (s3_ref, c3_ref)):
            count = s_ref.shape[0] // CHUNKS
            for c in range(count):
                for q in range(SLOTS // 2):
                    c_ref[step * count + c, :, q * 128 : (q + 1) * 128] = jnp.concatenate(
                        [s_ref[step * count + c, 2 * q], s_ref[step * count + c, 2 * q + 1]], axis=1
                    )


def near_kernel(n0, leaf, cols, near_src_hbm, x_hbm, blocks_hbm, after_ref, near_ref, x_ref, near_src_ref, blocks_ref, sems, block_sems):
    del after_ref
    small = copies([(near_src_hbm, near_src_ref), (x_hbm, x_ref.at[:, pl.ds(0, n0 * leaf)])], sems)

    def chunk(step):
        span = pl.ds(step * (n0 // STEPS), n0 // STEPS)
        return pltpu.make_async_copy(blocks_hbm.at[span], blocks_ref.at[span], block_sems.at[step])

    for c in small:
        c.start()
    for step in range(STEPS):
        chunk(step).start()
    x_ref[:, n0 * leaf :] = jnp.zeros((x_ref.shape[0], leaf), jnp.bfloat16)
    for c in small:
        c.wait()
    first_leaf = (lax.axis_index("row") * cols + lax.axis_index("col")) * n0

    @pl.loop(0, STEPS)
    def _(step):
        chunk(step).wait()
        for j in range(n0 // STEPS):
            i = step * (n0 // STEPS) + j
            acc = None
            for s in range(2):
                at = near_src_ref[s, i] - first_leaf
                at = jnp.where((at >= 0) & (at < n0), at, n0)
                xs = x_ref[:, pl.ds(pl.multiple_of(at * leaf, leaf), leaf)]
                part = dot(xs, blocks_ref[i, s], NT)
                acc = part if acc is None else acc + part
            near_ref[:, pl.ds(pl.multiple_of(i * leaf, leaf), leaf)] = acc


def join_kernel(parts, core_ref, after_ref, *refs):
    del after_ref
    out_ref = refs[parts]
    size = refs[0].shape[0]
    for j in range(parts):
        out_ref[j * size : (j + 1) * size] = refs[j][...]
    out_ref[parts * size :] = core_ref[...]


def product_kernel(
    n0, leaf, cols, pairs, i0_ref, i1_ref, i2_ref, i3_ref, near_src_ref, a_ref, b_ref, c0_ref, c1_ref, c2_ref, c3_ref,
    e1_ref, e2_ref, e3_ref, basis_ref, near_ref, x_hbm, blocks_hbm, out_ref,
    table_ref, f0_ref, f1_ref, f2_ref, f3_ref, down_ref, x_ref, blocks_ref, outer_ref, sems,
):
    nrhs = out_ref.shape[0]
    low = low_half((nrhs, 128))
    chips = cols // 2
    width = HALO * leaf // 128
    block = pairs + 2 * width
    side = 2 * HALO * leaf
    ends = [pl.ds(0, HALO), pl.ds(n0 - HALO, HALO)]
    fetch = copies(
        [
            (x_hbm.at[:, pl.ds(0, side)], x_ref.at[:, pl.ds(HALO * leaf, side)]),
            (x_hbm.at[:, pl.ds(n0 * leaf - side, side)], x_ref.at[:, pl.ds(HALO * leaf + side, side)]),
            (blocks_hbm.at[ends[0]], blocks_ref.at[pl.ds(0, HALO)]),
            (blocks_hbm.at[ends[1]], blocks_ref.at[pl.ds(HALO, HALO)]),
        ],
        sems,
    )
    for c in fetch:
        c.start()

    @pl.loop(0, chips)
    def _(t):
        for h, ref in enumerate((a_ref, b_ref)):
            for j in range(pairs):
                v = ref[t * block + j]
                at = ((h * chips + t) * pairs + j) * 2
                table_ref[at] = v
                table_ref[at + 1] = jnp.concatenate([v[:, 64:], v[:, :64]], axis=1)

    table_ref[2 * cols * pairs] = jnp.zeros((nrhs, 128), jnp.bfloat16)
    table_ref[2 * cols * pairs + 1] = jnp.zeros((nrhs, 128), jnp.bfloat16)

    def couple(c_ref, spot, i):
        xs = [
            jnp.where(low, table_ref[spot(2 * q, i)], table_ref[spot(2 * q + 1, i)])
            for q in range(SLOTS // 2)
        ]
        return dot(c_ref[i], jnp.concatenate(xs, axis=1), NT)

    def by_slot(ref):
        return lambda k, i: ref[k, i]

    def by_row(ref):
        return lambda k, i: ref[i, k]

    @pl.loop(0, n0 // 8)
    def _(t):
        for per, c_ref, spot, f_ref in (
            (1, c3_ref, by_row(i3_ref), f3_ref),
            (2, c2_ref, by_row(i2_ref), f2_ref),
            (4, c1_ref, by_slot(i1_ref), f1_ref),
            (8, c0_ref, by_slot(i0_ref), f0_ref),
        ):
            for j in range(per):
                f_ref[t * per + j] = couple(c_ref, spot, t * per + j)

    row, col = lax.axis_index("row"), lax.axis_index("col")
    odd = col % 2
    across = col + 2 * odd - 1
    inside = (across >= 0) & (across < cols)
    chip = jnp.where(inside, (col ^ across) // 2, chips - 1)
    at_edge = chip * block + pairs + jnp.where(inside, 0, width)
    at_core = chips * block
    left = jnp.where(odd == 1, at_core, at_edge)
    right = jnp.where(odd == 1, at_edge, at_core)
    end = HALO * leaf + 2 * side
    for j in range(width):
        x_ref[:, j * 128 : (j + 1) * 128] = b_ref[left + j]
        x_ref[:, end + j * 128 : end + (j + 1) * 128] = b_ref[right + j]
    zero = 6 * HALO
    x_ref[:, zero * leaf :] = jnp.zeros((nrhs, leaf), jnp.bfloat16)
    for c in fetch:
        c.wait()
    first_leaf = (row * cols + col) * n0
    for j in range(2 * HALO):
        i = j if j < HALO else n0 - 2 * HALO + j
        shift = HALO if j < HALO else 5 * HALO - n0
        acc = None
        for s in range(2):
            src = near_src_ref[s, i]
            at = jnp.where(src >= 0, src - first_leaf + shift, zero)
            xs = x_ref[:, pl.ds(pl.multiple_of(at * leaf, leaf), leaf)]
            part = dot(xs, blocks_ref[j, s], NT)
            acc = part if acc is None else acc + part
        outer_ref[:, j * leaf : (j + 1) * leaf] = acc

    down = [f3_ref[p].astype(jnp.bfloat16) for p in range(n0 // 8)]
    for e_ref, f_ref in ((e3_ref, f2_ref), (e2_ref, f1_ref), (e1_ref, f0_ref)):
        below = []
        for p, d in enumerate(down):
            pair = dot(e_ref[p], d, NN)
            for h in range(2):
                below.append((f_ref[2 * p + h] + pair[h * 64 : (h + 1) * 64]).astype(jnp.bfloat16))
        down = below
    for i, d in enumerate(down):
        down_ref[i] = d

    batch = 8

    @pl.loop(0, n0 // batch)
    def _(t):
        for j in range(batch):
            i = t * batch + j
            far = dot(down_ref[i], basis_ref[t * (batch // 2) + j // 2, (j % 2) * 64 : (j % 2 + 1) * 64], TN)
            at = pl.ds(pl.multiple_of(i * leaf, leaf), leaf)
            out_ref[:, at] = (far + near_ref[:, at]).astype(jnp.bfloat16)

    for j in range(2 * HALO):
        i = j if j < HALO else n0 - 2 * HALO + j
        far = dot(down_ref[i], basis_ref[i // 2, (i % 2) * 64 : (i % 2 + 1) * 64], TN)
        out_ref[:, i * leaf : (i + 1) * leaf] = (far + outer_ref[:, j * leaf : (j + 1) * leaf]).astype(jnp.bfloat16)


def shards(
    points_rhs, leaf_basis, near_src, near_blocks, transfer_first, transfer_second, transfer_third,
    far_zero, far_one, far_two, far_three, couple_zero, couple_one, couple_two, couple_three,
):
    bf, f32, i32 = jnp.bfloat16, jnp.float32, jnp.int32
    n0, leaf, rank = leaf_basis.shape
    nrhs = points_rhs.shape[1]
    rows, cols = lax.axis_size("row"), lax.axis_size("col")
    n1, n2, n3 = n0 // 2, n0 // 4, n0 // 8
    x = points_rhs.T
    basis = leaf_basis.transpose(0, 2, 1).reshape(n1, 2 * rank, leaf)
    e1, e2, e3 = (
        e.reshape(e.shape[0] // 2, 2 * rank, rank) for e in (transfer_first, transfer_second, transfer_third)
    )
    own_pairs = (n0 + n1 + n2) // 2
    top_pairs = n3 // 2
    width = HALO * leaf // 128
    pairs = own_pairs + rows * top_pairs

    def blocks_of(n):
        return jax.ShapeDtypeStruct((n, nrhs, 2 * rank), bf)

    def params(mib):
        return pltpu.CompilerParams(vmem_limit_bytes=mib << 20)

    def cost(us):
        return pl.CostEstimate(flops=int(us * 2e8), bytes_accessed=int(us * 3e6), transcendentals=0)

    skel, near_row, far_row, chip, core = pl.pallas_call(
        functools.partial(upward_kernel, n0, leaf),
        out_shape=[blocks_of(own_pairs), blocks_of(top_pairs + width), blocks_of(top_pairs + width)]
        + [blocks_of(width)] * 2,
        in_specs=[HBM] * 5,
        out_specs=[VMEM] * 5,
        scratch_shapes=[pltpu.VMEM(v.shape, bf) for v in (x, basis, e1, e2, e3)]
        + [pltpu.SemaphoreType.DMA((4,)), pltpu.SemaphoreType.DMA((CHUNKS,))],
        compiler_params=params(12),
        cost_estimate=cost(2),
        name="upward",
    )(*map(in_hbm, (x, basis, e1, e2, e3)))

    def swap(v, axis, size, k):
        return lax.ppermute(v, axis, [(i, i ^ k) for i in range(size)])

    tops = [None] * rows
    for k in reversed(range(1, rows)):
        mersenne = (k & (k + 1)) == 0
        tops[k] = swap(near_row if k == 1 else far_row if mersenne else near_row[:top_pairs], "row", rows, k)

    lists = (far_zero.T, far_one.T, far_two, far_three)
    blocks = (couple_zero, couple_one, couple_two, couple_three)
    i0, i1, i2, i3, c0, c1, c2, c3 = pl.pallas_call(
        functools.partial(fold_kernel, n0, cols, rows),
        out_shape=[jax.ShapeDtypeStruct(f.shape, i32) for f in lists]
        + [jax.ShapeDtypeStruct((n, rank, SLOTS * rank), bf) for n in (n0, n1, n2, n3)],
        in_specs=[HBM] * 8,
        out_specs=[VMEM] * 8,
        scratch_shapes=[pltpu.VMEM(f.shape, i32) for f in lists]
        + [pltpu.VMEM(s.shape, bf) for s in blocks]
        + [pltpu.SemaphoreType.DMA((4,)), pltpu.SemaphoreType.DMA((CHUNKS, 4))],
        compiler_params=params(14),
        cost_estimate=cost(4),
        name="fold",
    )(*map(in_hbm, (*lists, *blocks)))

    mine = pl.pallas_call(
        functools.partial(pack_kernel, rows, cols, top_pairs),
        out_shape=blocks_of(pairs + 2 * width),
        in_specs=[VMEM, VMEM, ANY] + [VMEM] * rows,
        out_specs=VMEM,
        compiler_params=params(4),
        name="pack",
    )(skel, chip, i3, near_row, *tops[1:])

    parts = [None] * (cols // 2)
    parts[0] = mine
    for k in reversed(range(1, cols // 2)):
        parts[k] = swap(mine, "col", cols, 2 * k)

    near = pl.pallas_call(
        functools.partial(near_kernel, n0, leaf, cols),
        out_shape=jax.ShapeDtypeStruct((nrhs, n0 * leaf), f32),
        in_specs=[HBM] * 3 + [ANY],
        out_specs=VMEM,
        scratch_shapes=[
            pltpu.VMEM((nrhs, (n0 + 1) * leaf), bf),
            pltpu.SMEM((2, n0), i32),
            pltpu.VMEM(near_blocks.shape, bf),
            pltpu.SemaphoreType.DMA((2,)),
            pltpu.SemaphoreType.DMA((STEPS,)),
        ],
        compiler_params=params(14),
        cost_estimate=cost(6),
        name="near",
    )(*map(in_hbm, (near_src.T, x, near_blocks)), mine)

    ours = pl.pallas_call(
        functools.partial(join_kernel, cols // 2),
        out_shape=blocks_of(cols // 2 * mine.shape[0] + width),
        in_specs=[VMEM, ANY] + [VMEM] * (cols // 2),
        out_specs=VMEM,
        compiler_params=params(8),
        name="join",
    )(core, near, *parts)
    theirs = swap(ours, "col", cols, 1)

    out = pl.pallas_call(
        functools.partial(product_kernel, n0, leaf, cols, pairs),
        out_shape=jax.ShapeDtypeStruct((nrhs, n0 * leaf), bf),
        in_specs=[SMEM] * 5 + [VMEM] * 11 + [HBM] * 2,
        out_specs=VMEM,
        scratch_shapes=[pltpu.VMEM((2 * cols * pairs + 2, nrhs, 2 * rank), bf)]
        + [pltpu.VMEM((n, rank, nrhs), f32) for n in (n0, n1, n2, n3)]
        + [
            pltpu.VMEM((n0, rank, nrhs), bf),
            pltpu.VMEM((nrhs, (6 * HALO + 1) * leaf), bf),
            pltpu.VMEM((2 * HALO, *near_blocks.shape[1:]), bf),
            pltpu.VMEM((nrhs, 2 * HALO * leaf), f32),
            pltpu.SemaphoreType.DMA((4,)),
        ],
        compiler_params=params(32),
        cost_estimate=cost(5),
        name="product",
    )(i0, i1, i2, i3, near_src.T, ours, theirs, c0, c1, c2, c3, e1, e2, e3, basis, near, *map(in_hbm, (x, near_blocks)))
    return out.T


def solution(mesh):
    whole = P(("row", "col"))
    return jax.shard_map(
        shards,
        mesh=mesh,
        in_specs=(whole,) * 15,
        out_specs=whole,
        check_vma=False,
    )
```

```python
import functools

import jax
import jax.numpy as jnp
from jax import lax
from jax.experimental import pallas as pl
from jax.experimental.pallas import tpu as pltpu
from jax.sharding import PartitionSpec as P


SLOTS = 8
HALO = 2
STEPS = 8
CHUNKS = 4
SENDS = 2


NT = (((1,), (1,)), ((), ()))
NN = (((1,), (0,)), ((), ()))
TN = (((0,), (0,)), ((), ()))

VMEM = pl.BlockSpec(memory_space=pltpu.VMEM)
SMEM = pl.BlockSpec(memory_space=pltpu.SMEM)
HBM = pl.BlockSpec(memory_space=pltpu.HBM)
ANY = pl.BlockSpec(memory_space=pl.ANY)


def in_hbm(v):
    return pltpu.with_memory_space_constraint(v, pltpu.HBM)


def dot(a, b, dims):
    return lax.dot_general(a, b, dims, preferred_element_type=jnp.float32)


def low_half(shape):
    return lax.broadcasted_iota(jnp.int32, shape, len(shape) - 1) < shape[-1] // 2


def copies(pairs, sems):
    return [pltpu.make_async_copy(src, dst, sems.at[i]) for i, (src, dst) in enumerate(pairs)]


def edge_blocks(ref, x_ref, at, width, first):
    for b in range(width // 128):
        ref[first + b] = x_ref[:, at + b * 128 : at + (b + 1) * 128]


def upward_kernel(
    n0, leaf, x_hbm, basis_hbm, e1_hbm, e2_hbm, e3_hbm, skel_ref, near_row_ref, far_row_ref, chip_ref, core_ref,
    x_ref, basis_ref, e1_ref, e2_ref, e3_ref, sems, basis_sems,
):
    chunk = n0 // 2 // CHUNKS
    top = n0 // 16
    width = HALO * leaf
    fetch = copies([(x_hbm, x_ref), (e1_hbm, e1_ref), (e2_hbm, e2_ref), (e3_hbm, e3_ref)], sems)
    spans = [pl.ds(c * chunk, chunk) for c in range(CHUNKS)]
    fetch_basis = copies([(basis_hbm.at[s], basis_ref.at[s]) for s in spans], basis_sems)
    fetch[0].start()
    for c in fetch_basis:
        c.start()
    for c in fetch[1:]:
        c.start()
    fetch[0].wait()

    def edges(even, head_to, tail_to):
        @pl.when(even)
        def _():
            edge_blocks(head_to[0], x_ref, 0, width, head_to[1])
            edge_blocks(tail_to[0], x_ref, n0 * leaf - width, width, tail_to[1])

        @pl.when(jnp.logical_not(even))
        def _():
            edge_blocks(tail_to[0], x_ref, 0, width, tail_to[1])
            edge_blocks(head_to[0], x_ref, n0 * leaf - width, width, head_to[1])

    edges(lax.axis_index("row") % 2 == 0, (far_row_ref, top), (near_row_ref, top))
    edges(lax.axis_index("col") % 2 == 0, (chip_ref, 0), (core_ref, 0))
    nrhs = x_ref.shape[0]
    low = low_half((nrhs, 128))
    level = []
    for p in range(n0 // 2):
        if p % chunk == 0:
            fetch_basis[p // chunk].wait()
        xs = jnp.concatenate([x_ref[:, (2 * p + h) * leaf : (2 * p + h + 1) * leaf] for h in range(2)], axis=0)
        both = dot(xs, basis_ref[p], NT)
        level.append(jnp.where(low, both[:nrhs], both[nrhs:]).astype(jnp.bfloat16))
        skel_ref[p] = level[p]
    base = n0 // 2
    for step, e_ref in enumerate((e1_ref, e2_ref, e3_ref)):
        fetch[1 + step].wait()
        parents = [dot(v, e_ref[p], NN) for p, v in enumerate(level)]
        level = [
            jnp.concatenate([parents[2 * q], parents[2 * q + 1]], axis=1).astype(jnp.bfloat16)
            for q in range(len(parents) // 2)
        ]
        for q, v in enumerate(level):
            if step < 2:
                skel_ref[base + q] = v
            else:
                near_row_ref[q] = v
                far_row_ref[q] = v
        base += len(level)


def pack_kernel(rows, cols, top, skel_ref, chip_ref, after_ref, own_ref, *refs):
    del after_ref
    own, width = skel_ref.shape[0], chip_ref.shape[0]
    tops, mine_ref = (own_ref, *reversed(refs[: rows - 1])), refs[rows - 1]
    mine_ref[:own] = skel_ref[...]
    for k in range(rows):
        mine_ref[own + k * top : own + (k + 1) * top] = tops[k][:top]
    base = own + rows * top
    mine_ref[base : base + width] = chip_ref[...]
    row, col = lax.axis_index("row"), lax.axis_index("col")
    odd = row % 2
    from_near = (col == cols - 1) == (odd == 1)
    partner = jnp.where(from_near, 1, row ^ (row + 2 * odd - 1))
    for m in range(1, rows.bit_length()):
        k = 2**m - 1
        if k >= rows:
            break

        @pl.when((partner == k) | (k == 1))
        def _(k=k):
            mine_ref[base + width :] = tops[k][top:]


def side_by_side(s_ref, i, c_ref, at):
    for q in range(SLOTS // 2):
        c_ref[at, :, q * 128 : (q + 1) * 128] = jnp.concatenate([s_ref[i, 2 * q], s_ref[i, 2 * q + 1]], axis=1)


def fold_kernel(
    n0, cols, rows, f0_hbm, f1_hbm, f2_hbm, f3_hbm, s1_hbm, s2_hbm, s3_hbm,
    i0_ref, i1_ref, i2_ref, i3_ref, c_ref, f0_ref, f1_ref, f2_ref, f3_ref, s1_ref, s2_ref, s3_ref, sems, block_sems,
):
    row, col = lax.axis_index("row"), lax.axis_index("col")
    pairs = (n0 // 2 + n0 // 4 + n0 // 8) + rows * (n0 // 16)
    lists = copies([(f0_hbm, f0_ref), (f1_hbm, f1_ref), (f2_hbm, f2_ref), (f3_hbm, f3_ref)], sems)
    n3 = n0 // 8
    streams = ((s3_hbm, s3_ref), (s2_hbm, s2_ref), (s1_hbm, s1_ref))

    def chunk(step):
        out = []
        for n, (src, dst) in enumerate(streams):
            size = src.shape[0] // CHUNKS
            span = pl.ds(step * size, size)
            out.append(pltpu.make_async_copy(src.at[span], dst.at[span], block_sems.at[step, n]))
        return out

    for c in lists:
        c.start()
    for step in range(CHUNKS):
        for c in chunk(step):
            c.start()
    for c in lists:
        c.wait()

    def place(f, slot_axis, per, first_pair, kz):
        dev = f // per
        pos = f % per
        k = (dev % cols) ^ col
        if kz:
            first_pair = first_pair + ((dev // cols) ^ row) * (per // 2)
        block = (k % 2) * (cols // 2) + k // 2
        spot = (block * pairs + first_pair) * 2 + pos
        slot = lax.broadcasted_iota(jnp.int32, f.shape, slot_axis)
        spot = spot ^ (slot % 2)
        return jnp.where(f >= 0, spot, cols * pairs * 2)

    i0_ref[...] = place(f0_ref[...], 0, n0, 0, False)
    i1_ref[...] = place(f1_ref[...], 0, n0 // 2, n0 // 2, False)
    i2_ref[...] = place(f2_ref[...], 1, n0 // 4, n0 // 2 + n0 // 4, False)
    i3_ref[...] = place(f3_ref[...], 1, n0 // 8, n0 // 2 + n0 // 4 + n0 // 8, True)

    @pl.loop(0, CHUNKS)
    def _(step):
        for c in chunk(step):
            c.wait()
        for s_ref, first in ((s3_ref, 0), (s2_ref, n3), (s1_ref, 3 * n3)):
            count = s_ref.shape[0] // CHUNKS
            for j in range(count):
                side_by_side(s_ref, step * count + j, c_ref, first + step * count + j)


def near_kernel(
    n0, leaf, cols, near_src_hbm, x_hbm, blocks_hbm, s_hbm, after_ref, near_ref, c_ref,
    x_ref, near_src_ref, blocks_ref, s_ref, sems, block_sems,
):
    del after_ref
    small = copies([(near_src_hbm, near_src_ref), (x_hbm, x_ref.at[:, pl.ds(0, n0 * leaf)])], sems)

    streams = ((blocks_hbm, blocks_ref), (s_hbm, s_ref))

    def chunk(step):
        span = pl.ds(step * (n0 // STEPS), n0 // STEPS)
        return copies([(src.at[span], dst.at[span]) for src, dst in streams], block_sems.at[step])

    for c in small:
        c.start()
    for step in range(STEPS):
        for c in chunk(step):
            c.start()
    x_ref[:, n0 * leaf :] = jnp.zeros((x_ref.shape[0], leaf), jnp.bfloat16)
    for c in small:
        c.wait()
    first_leaf = (lax.axis_index("row") * cols + lax.axis_index("col")) * n0

    @pl.loop(0, STEPS)
    def _(step):
        for c in chunk(step):
            c.wait()
        for j in range(n0 // STEPS):
            i = step * (n0 // STEPS) + j
            side_by_side(s_ref, i, c_ref, i)
            acc = None
            for s in range(2):
                at = near_src_ref[s, i] - first_leaf
                at = jnp.where((at >= 0) & (at < n0), at, n0)
                xs = x_ref[:, pl.ds(pl.multiple_of(at * leaf, leaf), leaf)]
                part = dot(xs, blocks_ref[i, s], NT)
                acc = part if acc is None else acc + part
            near_ref[:, pl.ds(pl.multiple_of(i * leaf, leaf), leaf)] = acc


def join_kernel(parts, core_ref, after_ref, *refs):
    del after_ref
    out_ref = refs[parts]
    size = refs[0].shape[0]
    for j in range(parts):
        out_ref[j * size : (j + 1) * size] = refs[j][...]
    out_ref[parts * size :] = core_ref[...]


def product_kernel(
    n0, leaf, cols, pairs, i0_hbm, i1_hbm, i2_hbm, i3_hbm, near_src_hbm, a_ref, b_ref, c_ref, c0_ref,
    e1_hbm, e2_hbm, e3_hbm, basis_ref, near_in_ref, x_hbm, blocks_hbm, out_hbm, near_ref,
    i0_ref, i1_ref, i2_ref, i3_ref, near_src_ref, table_ref, field_ref, down_ref, e_ref, x_ref, blocks_ref, out_ref,
    list_sems, sems, out_sems,
):
    del near_in_ref
    nrhs = out_ref.shape[0]
    low = low_half((nrhs, 128))
    chips = cols // 2
    width = HALO * leaf // 128
    block = pairs + 2 * width
    side = 2 * HALO * leaf
    n1, n2, n3 = n0 // 2, n0 // 4, n0 // 8
    ends = [pl.ds(0, HALO), pl.ds(n0 - HALO, HALO)]
    lists = copies(
        [
            (i0_hbm, i0_ref), (i1_hbm, i1_ref), (i2_hbm, i2_ref), (i3_hbm, i3_ref), (near_src_hbm, near_src_ref),
        ],
        list_sems,
    )
    fetch = copies(
        [
            (x_hbm.at[:, pl.ds(0, side)], x_ref.at[:, pl.ds(HALO * leaf, side)]),
            (x_hbm.at[:, pl.ds(n0 * leaf - side, side)], x_ref.at[:, pl.ds(HALO * leaf + side, side)]),
            (blocks_hbm.at[ends[0]], blocks_ref.at[pl.ds(0, HALO)]),
            (blocks_hbm.at[ends[1]], blocks_ref.at[pl.ds(HALO, HALO)]),
            (e3_hbm, e_ref.at[pl.ds(0, n3)]),
            (e2_hbm, e_ref.at[pl.ds(n3, n2)]),
            (e1_hbm, e_ref.at[pl.ds(n3 + n2, n1)]),
        ],
        sems,
    )
    for f in lists + fetch:
        f.start()

    parts = 1
    wide = pairs // parts

    @pl.loop(0, chips * parts)
    def _(t):
        chip, part = t // parts, t % parts
        for h, ref in enumerate((a_ref, b_ref)):
            for j in range(wide):
                v = ref[chip * block + part * wide + j]
                at = ((h * chips + chip) * pairs + part * wide + j) * 2
                table_ref[at] = v
                table_ref[at + 1] = jnp.concatenate([v[:, 64:], v[:, :64]], axis=1)

    table_ref[2 * cols * pairs] = jnp.zeros((nrhs, 128), jnp.bfloat16)
    table_ref[2 * cols * pairs + 1] = jnp.zeros((nrhs, 128), jnp.bfloat16)
    for f in lists:
        f.wait()

    @pl.loop(0, n3)
    def _(t):
        for per, first, spot in (
            (1, 0, lambda k, i: i3_ref[i, k]),
            (2, n3, lambda k, i: i2_ref[i, k]),
            (4, n3 + n2, lambda k, i: i1_ref[k, i]),
            (8, n3 + n2 + n1, lambda k, i: i0_ref[k, i]),
        ):
            for j in range(per):
                i = t * per + j
                xs = [
                    jnp.where(low, table_ref[spot(2 * q, i)], table_ref[spot(2 * q + 1, i)])
                    for q in range(SLOTS // 2)
                ]
                blocks = c_ref[first + i] if per < 8 else c0_ref[i]
                field_ref[first + i] = dot(blocks, jnp.concatenate(xs, axis=1), NT)

    row, col = lax.axis_index("row"), lax.axis_index("col")
    odd = col % 2
    across = col + 2 * odd - 1
    inside = (across >= 0) & (across < cols)
    chip = jnp.where(inside, (col ^ across) // 2, chips - 1)
    at_edge = chip * block + pairs + jnp.where(inside, 0, width)
    at_core = chips * block
    left = jnp.where(odd == 1, at_core, at_edge)
    right = jnp.where(odd == 1, at_edge, at_core)
    end = HALO * leaf + 2 * side
    for j in range(width):
        x_ref[:, j * 128 : (j + 1) * 128] = b_ref[left + j]
        x_ref[:, end + j * 128 : end + (j + 1) * 128] = b_ref[right + j]
    zero = 6 * HALO
    x_ref[:, zero * leaf :] = jnp.zeros((nrhs, leaf), jnp.bfloat16)
    for f in fetch:
        f.wait()
    first_leaf = (row * cols + col) * n0

    for j in range(HALO):
        for b, i, shift in ((j, j, HALO), (HALO + j, n0 - HALO + j, 5 * HALO - n0)):
            acc = None
            for s in range(2):
                src = near_src_ref[s, i]
                at = jnp.where(src >= 0, src - first_leaf + shift, zero)
                xs = x_ref[:, pl.ds(pl.multiple_of(at * leaf, leaf), leaf)]
                part = dot(xs, blocks_ref[b, s], NT)
                acc = part if acc is None else acc + part
            near_ref[:, pl.ds(pl.multiple_of(i * leaf, leaf), leaf)] = acc

    down = [field_ref[p].astype(jnp.bfloat16) for p in range(n3)]
    for p in range(7 * n3):
        pair = dot(e_ref[p], down[p], NN)
        for h in range(2):
            c = n3 + 2 * p + h
            down.append((field_ref[c] + pair[h * 64 : (h + 1) * 64]).astype(jnp.bfloat16))
    for i in range(n0):
        down_ref[i] = down[7 * n3 + i]

    def send(t):
        span = pl.ds(pl.multiple_of(t * n0 // SENDS * leaf, leaf), n0 // SENDS * leaf)
        return pltpu.make_async_copy(out_ref.at[:, span], out_hbm.at[:, span], out_sems.at[t])

    @pl.loop(0, SENDS)
    def _(t):
        for j in range(n0 // SENDS):
            i = t * (n0 // SENDS) + j
            d = down_ref[i]
            far = dot(d, basis_ref[t * (n1 // SENDS) + j // 2, (j % 2) * 64 : (j % 2 + 1) * 64], TN)
            at = pl.ds(pl.multiple_of(i * leaf, leaf), leaf)
            out_ref[:, at] = (far + near_ref[:, at]).astype(jnp.bfloat16)
        send(t).start()

    for t in range(SENDS):
        send(t).wait()


def shards(
    points_rhs, leaf_basis, near_src, near_blocks, transfer_first, transfer_second, transfer_third,
    far_zero, far_one, far_two, far_three, couple_zero, couple_one, couple_two, couple_three,
):
    bf, f32, i32 = jnp.bfloat16, jnp.float32, jnp.int32
    n0, leaf, rank = leaf_basis.shape
    nrhs = points_rhs.shape[1]
    rows, cols = lax.axis_size("row"), lax.axis_size("col")
    n1, n2, n3 = n0 // 2, n0 // 4, n0 // 8
    x = points_rhs.T
    basis = leaf_basis.transpose(0, 2, 1).reshape(n1, 2 * rank, leaf)
    e1, e2, e3 = (
        e.reshape(e.shape[0] // 2, 2 * rank, rank) for e in (transfer_first, transfer_second, transfer_third)
    )
    own_pairs = (n0 + n1 + n2) // 2
    top_pairs = n3 // 2
    width = HALO * leaf // 128
    pairs = own_pairs + rows * top_pairs

    def blocks_of(n):
        return jax.ShapeDtypeStruct((n, nrhs, 2 * rank), bf)

    def params(mib):
        return pltpu.CompilerParams(vmem_limit_bytes=mib << 20)

    def cost(us):
        return pl.CostEstimate(flops=int(us * 2e8), bytes_accessed=int(us * 3e6), transcendentals=0)

    skel, near_row, far_row, chip, core = pl.pallas_call(
        functools.partial(upward_kernel, n0, leaf),
        out_shape=[blocks_of(own_pairs), blocks_of(top_pairs + width), blocks_of(top_pairs + width)]
        + [blocks_of(width)] * 2,
        in_specs=[HBM] * 5,
        out_specs=[VMEM] * 5,
        scratch_shapes=[pltpu.VMEM(v.shape, bf) for v in (x, basis, e1, e2, e3)]
        + [pltpu.SemaphoreType.DMA((4,)), pltpu.SemaphoreType.DMA((CHUNKS,))],
        compiler_params=params(12),
        cost_estimate=cost(2),
        name="upward",
    )(*map(in_hbm, (x, basis, e1, e2, e3)))

    def swap(v, axis, size, k):
        return lax.ppermute(v, axis, [(i, i ^ k) for i in range(size)])

    tops = [None] * rows
    for k in reversed(range(1, rows)):
        mersenne = (k & (k + 1)) == 0
        sent = near_row if k == 1 else far_row if mersenne else near_row[:top_pairs]
        tops[k] = swap(sent, "row", rows, k)

    lists = (far_zero.T, far_one.T, far_two, far_three)
    blocks = (couple_one, couple_two, couple_three)
    i0, i1, i2, i3, c = pl.pallas_call(
        functools.partial(fold_kernel, n0, cols, rows),
        out_shape=[jax.ShapeDtypeStruct(f.shape, i32) for f in lists]
        + [jax.ShapeDtypeStruct((7 * n3, rank, SLOTS * rank), bf)],
        in_specs=[HBM] * 7,
        out_specs=[VMEM] * 5,
        scratch_shapes=[pltpu.VMEM(f.shape, i32) for f in lists]
        + [pltpu.VMEM(s.shape, bf) for s in blocks]
        + [pltpu.SemaphoreType.DMA((4,)), pltpu.SemaphoreType.DMA((CHUNKS, 3))],
        compiler_params=params(14),
        cost_estimate=cost(4),
        name="fold",
    )(*map(in_hbm, (*lists, *blocks)))

    mine = pl.pallas_call(
        functools.partial(pack_kernel, rows, cols, top_pairs),
        out_shape=blocks_of(pairs + 2 * width),
        in_specs=[VMEM, VMEM, ANY] + [VMEM] * rows,
        out_specs=VMEM,
        compiler_params=params(4),
        name="pack",
    )(skel, chip, i3, near_row, *reversed(tops[1:]))

    parts = [None] * (cols // 2)
    parts[0] = mine
    for k in reversed(range(1, cols // 2)):
        parts[k] = swap(mine, "col", cols, 2 * k)

    near, c0 = pl.pallas_call(
        functools.partial(near_kernel, n0, leaf, cols),
        out_shape=[
            jax.ShapeDtypeStruct((nrhs, n0 * leaf), f32),
            jax.ShapeDtypeStruct((n0, rank, SLOTS * rank), bf),
        ],
        in_specs=[HBM] * 4 + [ANY],
        out_specs=[VMEM] * 2,
        scratch_shapes=[
            pltpu.VMEM((nrhs, (n0 + 1) * leaf), bf),
            pltpu.SMEM((2, n0), i32),
            pltpu.VMEM(near_blocks.shape, bf),
            pltpu.VMEM(couple_zero.shape, bf),
            pltpu.SemaphoreType.DMA((2,)),
            pltpu.SemaphoreType.DMA((STEPS, 2)),
        ],
        compiler_params=params(18),
        cost_estimate=cost(6),
        name="near",
    )(*map(in_hbm, (near_src.T, x, near_blocks, couple_zero)), mine)

    ours = pl.pallas_call(
        functools.partial(join_kernel, cols // 2),
        out_shape=blocks_of(cols // 2 * mine.shape[0] + width),
        in_specs=[VMEM, ANY] + [VMEM] * (cols // 2),
        out_specs=VMEM,
        compiler_params=params(8),
        name="join",
    )(core, near, *parts)
    theirs = swap(ours, "col", cols, 1)

    out, _ = pl.pallas_call(
        functools.partial(product_kernel, n0, leaf, cols, pairs),
        out_shape=[jax.ShapeDtypeStruct((nrhs, n0 * leaf), bf), jax.ShapeDtypeStruct((nrhs, n0 * leaf), f32)],
        in_specs=[ANY] * 4 + [HBM] + [VMEM] * 4 + [HBM] * 3 + [VMEM] * 2 + [HBM] * 2,
        out_specs=[HBM, VMEM],
        input_output_aliases={13: 1},
        scratch_shapes=[pltpu.SMEM(v.shape, i32) for v in (i0, i1, i2, i3, near_src.T)]
        + [
            pltpu.VMEM((2 * cols * pairs + 2, nrhs, 2 * rank), bf),
            pltpu.VMEM((15 * n3, rank, nrhs), f32),
            pltpu.VMEM((n0, rank, nrhs), bf),
            pltpu.VMEM((7 * n3, 2 * rank, rank), bf),
            pltpu.VMEM((nrhs, (6 * HALO + 1) * leaf), bf),
            pltpu.VMEM((2 * HALO, *near_blocks.shape[1:]), bf),
            pltpu.VMEM((nrhs, n0 * leaf), bf),
            pltpu.SemaphoreType.DMA((5,)),
            pltpu.SemaphoreType.DMA((7,)),
            pltpu.SemaphoreType.DMA((SENDS,)),
        ],
        compiler_params=params(28),
        cost_estimate=cost(5),
        name="product",
    )(
        i0, i1, i2, i3, in_hbm(near_src.T), ours, theirs, c, c0, *map(in_hbm, (e1, e2, e3)), basis, near,
        *map(in_hbm, (x, near_blocks)),
    )
    return out.T


def solution(mesh):
    whole = P(("row", "col"))
    return jax.shard_map(
        shards,
        mesh=mesh,
        in_specs=(whole,) * 15,
        out_specs=whole,
        check_vma=False,
    )
```

```python
import functools

import jax
import jax.numpy as jnp
from jax import lax
from jax.experimental import pallas as pl
from jax.experimental.pallas import tpu as pltpu
from jax.sharding import PartitionSpec as P


SLOTS = 8
HALO = 2
STEPS = 2
CHUNKS = 2
SENDS = 1


NT = (((1,), (1,)), ((), ()))
NN = (((1,), (0,)), ((), ()))
TN = (((0,), (0,)), ((), ()))

VMEM = pl.BlockSpec(memory_space=pltpu.VMEM)
SMEM = pl.BlockSpec(memory_space=pltpu.SMEM)
HBM = pl.BlockSpec(memory_space=pltpu.HBM)
ANY = pl.BlockSpec(memory_space=pl.ANY)


def in_hbm(v):
    return pltpu.with_memory_space_constraint(v, pltpu.HBM)


def dot(a, b, dims):
    return lax.dot_general(a, b, dims, preferred_element_type=jnp.float32)


def low_half(shape):
    return lax.broadcasted_iota(jnp.int32, shape, len(shape) - 1) < shape[-1] // 2


def copies(pairs, sems):
    return [pltpu.make_async_copy(src, dst, sems.at[i]) for i, (src, dst) in enumerate(pairs)]


def edge_blocks(ref, x_ref, at, width, first):
    for b in range(width // 128):
        ref[first + b] = x_ref[:, at + b * 128 : at + (b + 1) * 128]


def upward_kernel(
    n0, leaf, x_hbm, basis_hbm, e1_hbm, e2_hbm, e3_hbm, skel_ref, near_row_ref, far_row_ref, chip_ref, core_ref,
    x_ref, basis_ref, e1_ref, e2_ref, e3_ref, sems, basis_sems,
):
    chunk = n0 // 2 // CHUNKS
    top = n0 // 16
    width = HALO * leaf
    fetch = copies([(x_hbm, x_ref), (e1_hbm, e1_ref), (e2_hbm, e2_ref), (e3_hbm, e3_ref)], sems)
    spans = [pl.ds(c * chunk, chunk) for c in range(CHUNKS)]
    fetch_basis = copies([(basis_hbm.at[s], basis_ref.at[s]) for s in spans], basis_sems)
    fetch[0].start()
    for c in fetch_basis:
        c.start()
    for c in fetch[1:]:
        c.start()
    fetch[0].wait()

    def edges(even, head_to, tail_to):
        @pl.when(even)
        def _():
            edge_blocks(head_to[0], x_ref, 0, width, head_to[1])
            edge_blocks(tail_to[0], x_ref, n0 * leaf - width, width, tail_to[1])

        @pl.when(jnp.logical_not(even))
        def _():
            edge_blocks(tail_to[0], x_ref, 0, width, tail_to[1])
            edge_blocks(head_to[0], x_ref, n0 * leaf - width, width, head_to[1])

    edges(lax.axis_index("row") % 2 == 0, (far_row_ref, top), (near_row_ref, top))
    edges(lax.axis_index("col") % 2 == 0, (chip_ref, 0), (core_ref, 0))
    nrhs = x_ref.shape[0]
    low = low_half((nrhs, 128))
    level = []
    for p in range(n0 // 2):
        if p % chunk == 0:
            fetch_basis[p // chunk].wait()
        xs = jnp.concatenate([x_ref[:, (2 * p + h) * leaf : (2 * p + h + 1) * leaf] for h in range(2)], axis=0)
        both = dot(xs, basis_ref[p], NT)
        level.append(jnp.where(low, both[:nrhs], both[nrhs:]).astype(jnp.bfloat16))
        skel_ref[p] = level[p]
    base = n0 // 2
    for step, e_ref in enumerate((e1_ref, e2_ref, e3_ref)):
        fetch[1 + step].wait()
        parents = [dot(v, e_ref[p], NN) for p, v in enumerate(level)]
        level = [
            jnp.concatenate([parents[2 * q], parents[2 * q + 1]], axis=1).astype(jnp.bfloat16)
            for q in range(len(parents) // 2)
        ]
        for q, v in enumerate(level):
            if step < 2:
                skel_ref[base + q] = v
            else:
                near_row_ref[q] = v
                far_row_ref[q] = v
        base += len(level)


def pack_kernel(rows, cols, top, skel_ref, chip_ref, after_ref, own_ref, *refs):
    del after_ref
    own, width = skel_ref.shape[0], chip_ref.shape[0]
    tops, mine_ref = (own_ref, *reversed(refs[: rows - 1])), refs[rows - 1]
    mine_ref[:own] = skel_ref[...]
    for k in range(rows):
        mine_ref[own + k * top : own + (k + 1) * top] = tops[k][:top]
    base = own + rows * top
    mine_ref[base : base + width] = chip_ref[...]
    row, col = lax.axis_index("row"), lax.axis_index("col")
    odd = row % 2
    from_near = (col == cols - 1) == (odd == 1)
    partner = jnp.where(from_near, 1, row ^ (row + 2 * odd - 1))
    for m in range(1, rows.bit_length()):
        k = 2**m - 1
        if k >= rows:
            break

        @pl.when((partner == k) | (k == 1))
        def _(k=k):
            mine_ref[base + width :] = tops[k][top:]


def side_by_side(s_ref, i, c_ref, at):
    for q in range(SLOTS // 2):
        c_ref[at, :, q * 128 : (q + 1) * 128] = jnp.concatenate([s_ref[i, 2 * q], s_ref[i, 2 * q + 1]], axis=1)


def fold_kernel(
    n0, cols, rows, f0_hbm, f1_hbm, f2_hbm, f3_hbm, s1_hbm, s2_hbm, s3_hbm,
    i0_ref, i1_ref, i2_ref, i3_ref, c_ref, f0_ref, f1_ref, f2_ref, f3_ref, s1_ref, s2_ref, s3_ref, sems, block_sems,
):
    row, col = lax.axis_index("row"), lax.axis_index("col")
    pairs = (n0 // 2 + n0 // 4 + n0 // 8) + rows * (n0 // 16)
    lists = copies([(f0_hbm, f0_ref), (f1_hbm, f1_ref), (f2_hbm, f2_ref), (f3_hbm, f3_ref)], sems)
    n3 = n0 // 8
    streams = ((s3_hbm, s3_ref), (s2_hbm, s2_ref), (s1_hbm, s1_ref))

    def chunk(step):
        out = []
        for n, (src, dst) in enumerate(streams):
            size = src.shape[0] // CHUNKS
            span = pl.ds(step * size, size)
            out.append(pltpu.make_async_copy(src.at[span], dst.at[span], block_sems.at[step, n]))
        return out

    for c in lists:
        c.start()
    for step in range(CHUNKS):
        for c in chunk(step):
            c.start()
    for c in lists:
        c.wait()

    def place(f, slot_axis, per, first_pair, kz):
        dev = f // per
        pos = f % per
        k = (dev % cols) ^ col
        if kz:
            first_pair = first_pair + ((dev // cols) ^ row) * (per // 2)
        block = (k % 2) * (cols // 2) + k // 2
        spot = (block * pairs + first_pair) * 2 + pos
        slot = lax.broadcasted_iota(jnp.int32, f.shape, slot_axis)
        spot = spot ^ (slot % 2)
        return jnp.where(f >= 0, spot, cols * pairs * 2)

    i0_ref[...] = place(f0_ref[...], 0, n0, 0, False)
    i1_ref[...] = place(f1_ref[...], 0, n0 // 2, n0 // 2, False)
    i2_ref[...] = place(f2_ref[...], 1, n0 // 4, n0 // 2 + n0 // 4, False)
    i3_ref[...] = place(f3_ref[...], 1, n0 // 8, n0 // 2 + n0 // 4 + n0 // 8, True)

    @pl.loop(0, CHUNKS)
    def _(step):
        for c in chunk(step):
            c.wait()
        for s_ref, first in ((s3_ref, 0), (s2_ref, n3), (s1_ref, 3 * n3)):
            count = s_ref.shape[0] // CHUNKS
            for j in range(count):
                side_by_side(s_ref, step * count + j, c_ref, first + step * count + j)


def near_kernel(
    n0, leaf, cols, near_src_hbm, x_hbm, blocks_hbm, s_hbm, after_ref, near_ref, c_ref,
    x_ref, near_src_ref, blocks_ref, s_ref, sems, block_sems,
):
    del after_ref
    small = copies([(near_src_hbm, near_src_ref), (x_hbm, x_ref.at[:, pl.ds(0, n0 * leaf)])], sems)

    streams = ((blocks_hbm, blocks_ref), (s_hbm, s_ref))

    def chunk(step):
        span = pl.ds(step * (n0 // STEPS), n0 // STEPS)
        return copies([(src.at[span], dst.at[span]) for src, dst in streams], block_sems.at[step])

    for c in small:
        c.start()
    for step in range(STEPS):
        for c in chunk(step):
            c.start()
    x_ref[:, n0 * leaf :] = jnp.zeros((x_ref.shape[0], leaf), jnp.bfloat16)
    for c in small:
        c.wait()
    first_leaf = (lax.axis_index("row") * cols + lax.axis_index("col")) * n0

    @pl.loop(0, STEPS)
    def _(step):
        for c in chunk(step):
            c.wait()
        for j in range(n0 // STEPS):
            i = step * (n0 // STEPS) + j
            side_by_side(s_ref, i, c_ref, i)
            acc = None
            for s in range(2):
                at = near_src_ref[s, i] - first_leaf
                at = jnp.where((at >= 0) & (at < n0), at, n0)
                xs = x_ref[:, pl.ds(pl.multiple_of(at * leaf, leaf), leaf)]
                part = dot(xs, blocks_ref[i, s], NT)
                acc = part if acc is None else acc + part
            near_ref[:, pl.ds(pl.multiple_of(i * leaf, leaf), leaf)] = acc


def join_kernel(parts, core_ref, after_ref, *refs):
    del after_ref
    out_ref = refs[parts]
    size = refs[0].shape[0]
    for j in range(parts):
        out_ref[j * size : (j + 1) * size] = refs[j][...]
    out_ref[parts * size :] = core_ref[...]


def product_kernel(
    n0, leaf, cols, pairs, i0_hbm, i1_hbm, i2_hbm, i3_hbm, near_src_hbm, a_ref, b_ref, c_ref, c0_ref,
    e1_hbm, e2_hbm, e3_hbm, basis_ref, near_in_ref, x_hbm, blocks_hbm, out_hbm, near_ref,
    i0_ref, i1_ref, i2_ref, i3_ref, near_src_ref, table_ref, field_ref, down_ref, e_ref, x_ref, blocks_ref, out_ref,
    list_sems, sems, out_sems,
):
    del near_in_ref
    nrhs = out_ref.shape[0]
    low = low_half((nrhs, 128))
    chips = cols // 2
    width = HALO * leaf // 128
    block = pairs + 2 * width
    side = 2 * HALO * leaf
    n1, n2, n3 = n0 // 2, n0 // 4, n0 // 8
    ends = [pl.ds(0, HALO), pl.ds(n0 - HALO, HALO)]
    lists = copies(
        [
            (i0_hbm, i0_ref), (i1_hbm, i1_ref), (i2_hbm, i2_ref), (i3_hbm, i3_ref), (near_src_hbm, near_src_ref),
        ],
        list_sems,
    )
    fetch = copies(
        [
            (x_hbm.at[:, pl.ds(0, side)], x_ref.at[:, pl.ds(HALO * leaf, side)]),
            (x_hbm.at[:, pl.ds(n0 * leaf - side, side)], x_ref.at[:, pl.ds(HALO * leaf + side, side)]),
            (blocks_hbm.at[ends[0]], blocks_ref.at[pl.ds(0, HALO)]),
            (blocks_hbm.at[ends[1]], blocks_ref.at[pl.ds(HALO, HALO)]),
            (e3_hbm, e_ref.at[pl.ds(0, n3)]),
            (e2_hbm, e_ref.at[pl.ds(n3, n2)]),
            (e1_hbm, e_ref.at[pl.ds(n3 + n2, n1)]),
        ],
        sems,
    )
    for f in lists + fetch:
        f.start()

    parts = 1
    wide = pairs // parts

    @pl.loop(0, chips * parts)
    def _(t):
        chip, part = t // parts, t % parts
        for h, ref in enumerate((a_ref, b_ref)):
            for j in range(wide):
                v = ref[chip * block + part * wide + j]
                at = ((h * chips + chip) * pairs + part * wide + j) * 2
                table_ref[at] = v
                table_ref[at + 1] = jnp.concatenate([v[:, 64:], v[:, :64]], axis=1)

    table_ref[2 * cols * pairs] = jnp.zeros((nrhs, 128), jnp.bfloat16)
    table_ref[2 * cols * pairs + 1] = jnp.zeros((nrhs, 128), jnp.bfloat16)
    for f in lists:
        f.wait()

    @pl.loop(0, n3 // 2)
    def _(t):
        for per, first, spot in (
            (2, 0, lambda k, i: i3_ref[i, k]),
            (4, n3, lambda k, i: i2_ref[i, k]),
            (8, n3 + n2, lambda k, i: i1_ref[k, i]),
            (16, n3 + n2 + n1, lambda k, i: i0_ref[k, i]),
        ):
            for j in range(per):
                i = t * per + j
                xs = [
                    jnp.where(low, table_ref[spot(2 * q, i)], table_ref[spot(2 * q + 1, i)])
                    for q in range(SLOTS // 2)
                ]
                blocks = c_ref[first + i] if first < 7 * n3 else c0_ref[i]
                field_ref[first + i] = dot(blocks, jnp.concatenate(xs, axis=1), NT)

    row, col = lax.axis_index("row"), lax.axis_index("col")
    odd = col % 2
    across = col + 2 * odd - 1
    inside = (across >= 0) & (across < cols)
    chip = jnp.where(inside, (col ^ across) // 2, chips - 1)
    at_edge = chip * block + pairs + jnp.where(inside, 0, width)
    at_core = chips * block
    left = jnp.where(odd == 1, at_core, at_edge)
    right = jnp.where(odd == 1, at_edge, at_core)
    end = HALO * leaf + 2 * side
    for j in range(width):
        x_ref[:, j * 128 : (j + 1) * 128] = b_ref[left + j]
        x_ref[:, end + j * 128 : end + (j + 1) * 128] = b_ref[right + j]
    zero = 6 * HALO
    x_ref[:, zero * leaf :] = jnp.zeros((nrhs, leaf), jnp.bfloat16)
    for f in fetch:
        f.wait()
    first_leaf = (row * cols + col) * n0

    for j in range(HALO):
        for b, i, shift in ((j, j, HALO), (HALO + j, n0 - HALO + j, 5 * HALO - n0)):
            acc = None
            for s in range(2):
                src = near_src_ref[s, i]
                at = jnp.where(src >= 0, src - first_leaf + shift, zero)
                xs = x_ref[:, pl.ds(pl.multiple_of(at * leaf, leaf), leaf)]
                part = dot(xs, blocks_ref[b, s], NT)
                acc = part if acc is None else acc + part
            near_ref[:, pl.ds(pl.multiple_of(i * leaf, leaf), leaf)] = acc

    down = [field_ref[p].astype(jnp.bfloat16) for p in range(n3)]
    for p in range(7 * n3):
        pair = dot(e_ref[p], down[p], NN)
        for h in range(2):
            c = n3 + 2 * p + h
            down.append((field_ref[c] + pair[h * 64 : (h + 1) * 64]).astype(jnp.bfloat16))
    for i in range(n0):
        down_ref[i] = down[7 * n3 + i]

    def send(t):
        span = pl.ds(pl.multiple_of(t * n0 // SENDS * leaf, leaf), n0 // SENDS * leaf)
        return pltpu.make_async_copy(out_ref.at[:, span], out_hbm.at[:, span], out_sems.at[t])

    @pl.loop(0, SENDS)
    def _(t):
        for j in range(n0 // SENDS):
            i = t * (n0 // SENDS) + j
            d = down_ref[i]
            far = dot(d, basis_ref[t * (n1 // SENDS) + j // 2, (j % 2) * 64 : (j % 2 + 1) * 64], TN)
            at = pl.ds(pl.multiple_of(i * leaf, leaf), leaf)
            out_ref[:, at] = (far + near_ref[:, at]).astype(jnp.bfloat16)
        send(t).start()

    for t in range(SENDS):
        send(t).wait()


def shards(
    points_rhs, leaf_basis, near_src, near_blocks, transfer_first, transfer_second, transfer_third,
    far_zero, far_one, far_two, far_three, couple_zero, couple_one, couple_two, couple_three,
):
    bf, f32, i32 = jnp.bfloat16, jnp.float32, jnp.int32
    n0, leaf, rank = leaf_basis.shape
    nrhs = points_rhs.shape[1]
    rows, cols = lax.axis_size("row"), lax.axis_size("col")
    n1, n2, n3 = n0 // 2, n0 // 4, n0 // 8
    x = points_rhs.T
    basis = leaf_basis.transpose(0, 2, 1).reshape(n1, 2 * rank, leaf)
    e1, e2, e3 = (
        e.reshape(e.shape[0] // 2, 2 * rank, rank) for e in (transfer_first, transfer_second, transfer_third)
    )
    own_pairs = (n0 + n1 + n2) // 2
    top_pairs = n3 // 2
    width = HALO * leaf // 128
    pairs = own_pairs + rows * top_pairs

    def blocks_of(n):
        return jax.ShapeDtypeStruct((n, nrhs, 2 * rank), bf)

    def params(mib):
        return pltpu.CompilerParams(vmem_limit_bytes=mib << 20)

    def cost(us):
        return pl.CostEstimate(flops=int(us * 2e8), bytes_accessed=int(us * 3e6), transcendentals=0)

    skel, near_row, far_row, chip, core = pl.pallas_call(
        functools.partial(upward_kernel, n0, leaf),
        out_shape=[blocks_of(own_pairs), blocks_of(top_pairs + width), blocks_of(top_pairs + width)]
        + [blocks_of(width)] * 2,
        in_specs=[HBM] * 5,
        out_specs=[VMEM] * 5,
        scratch_shapes=[pltpu.VMEM(v.shape, bf) for v in (x, basis, e1, e2, e3)]
        + [pltpu.SemaphoreType.DMA((4,)), pltpu.SemaphoreType.DMA((CHUNKS,))],
        compiler_params=params(12),
        cost_estimate=cost(2),
        name="upward",
    )(*map(in_hbm, (x, basis, e1, e2, e3)))

    def swap(v, axis, size, k):
        return lax.ppermute(v, axis, [(i, i ^ k) for i in range(size)])

    tops = [None] * rows
    for k in reversed(range(1, rows)):
        mersenne = (k & (k + 1)) == 0
        sent = near_row if k == 1 else far_row if mersenne else near_row[:top_pairs]
        tops[k] = swap(sent, "row", rows, k)

    lists = (far_zero.T, far_one.T, far_two, far_three)
    blocks = (couple_one, couple_two, couple_three)
    i0, i1, i2, i3, c = pl.pallas_call(
        functools.partial(fold_kernel, n0, cols, rows),
        out_shape=[jax.ShapeDtypeStruct(f.shape, i32) for f in lists]
        + [jax.ShapeDtypeStruct((7 * n3, rank, SLOTS * rank), bf)],
        in_specs=[HBM] * 7,
        out_specs=[VMEM] * 5,
        scratch_shapes=[pltpu.VMEM(f.shape, i32) for f in lists]
        + [pltpu.VMEM(s.shape, bf) for s in blocks]
        + [pltpu.SemaphoreType.DMA((4,)), pltpu.SemaphoreType.DMA((CHUNKS, 3))],
        compiler_params=params(14),
        cost_estimate=cost(4),
        name="fold",
    )(*map(in_hbm, (*lists, *blocks)))

    mine = pl.pallas_call(
        functools.partial(pack_kernel, rows, cols, top_pairs),
        out_shape=blocks_of(pairs + 2 * width),
        in_specs=[VMEM, VMEM, ANY] + [VMEM] * rows,
        out_specs=VMEM,
        compiler_params=params(4),
        name="pack",
    )(skel, chip, i3, near_row, *reversed(tops[1:]))

    parts = [None] * (cols // 2)
    parts[0] = mine
    for k in reversed(range(1, cols // 2)):
        parts[k] = swap(mine, "col", cols, 2 * k)

    near, c0 = pl.pallas_call(
        functools.partial(near_kernel, n0, leaf, cols),
        out_shape=[
            jax.ShapeDtypeStruct((nrhs, n0 * leaf), f32),
            jax.ShapeDtypeStruct((n0, rank, SLOTS * rank), bf),
        ],
        in_specs=[HBM] * 4 + [ANY],
        out_specs=[VMEM] * 2,
        scratch_shapes=[
            pltpu.VMEM((nrhs, (n0 + 1) * leaf), bf),
            pltpu.SMEM((2, n0), i32),
            pltpu.VMEM(near_blocks.shape, bf),
            pltpu.VMEM(couple_zero.shape, bf),
            pltpu.SemaphoreType.DMA((2,)),
            pltpu.SemaphoreType.DMA((STEPS, 2)),
        ],
        compiler_params=params(18),
        cost_estimate=cost(6),
        name="near",
    )(*map(in_hbm, (near_src.T, x, near_blocks, couple_zero)), mine)

    ours = pl.pallas_call(
        functools.partial(join_kernel, cols // 2),
        out_shape=blocks_of(cols // 2 * mine.shape[0] + width),
        in_specs=[VMEM, ANY] + [VMEM] * (cols // 2),
        out_specs=VMEM,
        compiler_params=params(8),
        name="join",
    )(core, near, *parts)
    theirs = swap(ours, "col", cols, 1)

    out, _ = pl.pallas_call(
        functools.partial(product_kernel, n0, leaf, cols, pairs),
        out_shape=[jax.ShapeDtypeStruct((nrhs, n0 * leaf), bf), jax.ShapeDtypeStruct((nrhs, n0 * leaf), f32)],
        in_specs=[ANY] * 4 + [HBM] + [VMEM] * 4 + [HBM] * 3 + [VMEM] * 2 + [HBM] * 2,
        out_specs=[HBM, VMEM],
        input_output_aliases={13: 1},
        scratch_shapes=[pltpu.SMEM(v.shape, i32) for v in (i0, i1, i2, i3, near_src.T)]
        + [
            pltpu.VMEM((2 * cols * pairs + 2, nrhs, 2 * rank), bf),
            pltpu.VMEM((15 * n3, rank, nrhs), f32),
            pltpu.VMEM((n0, rank, nrhs), bf),
            pltpu.VMEM((7 * n3, 2 * rank, rank), bf),
            pltpu.VMEM((nrhs, (6 * HALO + 1) * leaf), bf),
            pltpu.VMEM((2 * HALO, *near_blocks.shape[1:]), bf),
            pltpu.VMEM((nrhs, n0 * leaf), bf),
            pltpu.SemaphoreType.DMA((5,)),
            pltpu.SemaphoreType.DMA((7,)),
            pltpu.SemaphoreType.DMA((SENDS,)),
        ],
        compiler_params=params(28),
        cost_estimate=cost(5),
        name="product",
    )(
        i0, i1, i2, i3, in_hbm(near_src.T), ours, theirs, c, c0, *map(in_hbm, (e1, e2, e3)), basis, near,
        *map(in_hbm, (x, near_blocks)),
    )
    return out.T


def solution(mesh):
    whole = P(("row", "col"))
    return jax.shard_map(
        shards,
        mesh=mesh,
        in_specs=(whole,) * 15,
        out_specs=whole,
        check_vma=False,
    )
```

```python
import functools

import jax
import jax.numpy as jnp
from jax import lax
from jax.experimental import pallas as pl
from jax.experimental.pallas import tpu as pltpu
from jax.sharding import PartitionSpec as P


SLOTS = 8
HALO = 2
STEPS = 2
CHUNKS = 2
SENDS = 1


NT = (((1,), (1,)), ((), ()))
NN = (((1,), (0,)), ((), ()))
TN = (((0,), (0,)), ((), ()))

VMEM = pl.BlockSpec(memory_space=pltpu.VMEM)
SMEM = pl.BlockSpec(memory_space=pltpu.SMEM)
HBM = pl.BlockSpec(memory_space=pltpu.HBM)
ANY = pl.BlockSpec(memory_space=pl.ANY)


def in_hbm(v):
    return pltpu.with_memory_space_constraint(v, pltpu.HBM)


def dot(a, b, dims):
    return lax.dot_general(a, b, dims, preferred_element_type=jnp.float32)


def low_half(shape):
    return lax.broadcasted_iota(jnp.int32, shape, len(shape) - 1) < shape[-1] // 2


def copies(pairs, sems):
    return [pltpu.make_async_copy(src, dst, sems.at[i]) for i, (src, dst) in enumerate(pairs)]


def edge_blocks(ref, x_ref, at, width, first):
    for b in range(width // 128):
        ref[first + b] = x_ref[:, at + b * 128 : at + (b + 1) * 128]


def upward_kernel(
    n0, leaf, x_hbm, basis_hbm, e1_hbm, e2_hbm, e3_hbm, skel_ref, near_row_ref, far_row_ref, chip_ref, core_ref,
    x_ref, basis_ref, e1_ref, e2_ref, e3_ref, sems, basis_sems,
):
    chunk = n0 // 2 // CHUNKS
    top = n0 // 16
    width = HALO * leaf
    fetch = copies([(x_hbm, x_ref), (e1_hbm, e1_ref), (e2_hbm, e2_ref), (e3_hbm, e3_ref)], sems)
    spans = [pl.ds(c * chunk, chunk) for c in range(CHUNKS)]
    fetch_basis = copies([(basis_hbm.at[s], basis_ref.at[s]) for s in spans], basis_sems)
    fetch[0].start()
    for c in fetch_basis:
        c.start()
    for c in fetch[1:]:
        c.start()
    fetch[0].wait()

    def edges(even, head_to, tail_to):
        @pl.when(even)
        def _():
            edge_blocks(head_to[0], x_ref, 0, width, head_to[1])
            edge_blocks(tail_to[0], x_ref, n0 * leaf - width, width, tail_to[1])

        @pl.when(jnp.logical_not(even))
        def _():
            edge_blocks(tail_to[0], x_ref, 0, width, tail_to[1])
            edge_blocks(head_to[0], x_ref, n0 * leaf - width, width, head_to[1])

    edges(lax.axis_index("row") % 2 == 0, (far_row_ref, top), (near_row_ref, top))
    edges(lax.axis_index("col") % 2 == 0, (chip_ref, 0), (core_ref, 0))
    nrhs = x_ref.shape[0]
    low = low_half((nrhs, 128))
    level = []
    for p in range(n0 // 2):
        if p % chunk == 0:
            fetch_basis[p // chunk].wait()
        xs = jnp.concatenate([x_ref[:, (2 * p + h) * leaf : (2 * p + h + 1) * leaf] for h in range(2)], axis=0)
        both = dot(xs, basis_ref[p], NT)
        level.append(jnp.where(low, both[:nrhs], both[nrhs:]).astype(jnp.bfloat16))
        skel_ref[p] = level[p]
    base = n0 // 2
    for step, e_ref in enumerate((e1_ref, e2_ref, e3_ref)):
        fetch[1 + step].wait()
        parents = [dot(v, e_ref[p], NN) for p, v in enumerate(level)]
        level = [
            jnp.concatenate([parents[2 * q], parents[2 * q + 1]], axis=1).astype(jnp.bfloat16)
            for q in range(len(parents) // 2)
        ]
        for q, v in enumerate(level):
            if step < 2:
                skel_ref[base + q] = v
            else:
                near_row_ref[q] = v
                far_row_ref[q] = v
        base += len(level)


def pack_kernel(rows, cols, top, skel_ref, chip_ref, after_ref, own_ref, *refs):
    del after_ref
    own, width = skel_ref.shape[0], chip_ref.shape[0]
    tops, mine_ref = (own_ref, *reversed(refs[: rows - 1])), refs[rows - 1]
    mine_ref[:own] = skel_ref[...]
    for k in range(rows):
        mine_ref[own + k * top : own + (k + 1) * top] = tops[k][:top]
    base = own + rows * top
    mine_ref[base : base + width] = chip_ref[...]
    row, col = lax.axis_index("row"), lax.axis_index("col")
    odd = row % 2
    from_near = (col == cols - 1) == (odd == 1)
    partner = jnp.where(from_near, 1, row ^ (row + 2 * odd - 1))
    for m in range(1, rows.bit_length()):
        k = 2**m - 1
        if k >= rows:
            break

        @pl.when((partner == k) | (k == 1))
        def _(k=k):
            mine_ref[base + width :] = tops[k][top:]


def side_by_side(s_ref, i, c_ref, at):
    for q in range(SLOTS // 2):
        c_ref[at, :, q * 128 : (q + 1) * 128] = jnp.concatenate([s_ref[i, 2 * q], s_ref[i, 2 * q + 1]], axis=1)


def fold_kernel(
    n0, cols, rows, f0_hbm, f1_hbm, f2_hbm, f3_hbm, s1_hbm, s2_hbm, s3_hbm,
    i0_ref, i1_ref, i2_ref, i3_ref, c_ref, f0_ref, f1_ref, f2_ref, f3_ref, s1_ref, s2_ref, s3_ref, sems, block_sems,
):
    row, col = lax.axis_index("row"), lax.axis_index("col")
    pairs = (n0 // 2 + n0 // 4 + n0 // 8) + rows * (n0 // 16)
    lists = copies([(f0_hbm, f0_ref), (f1_hbm, f1_ref), (f2_hbm, f2_ref), (f3_hbm, f3_ref)], sems)
    n3 = n0 // 8
    streams = ((s3_hbm, s3_ref), (s2_hbm, s2_ref), (s1_hbm, s1_ref))

    def chunk(step):
        out = []
        for n, (src, dst) in enumerate(streams):
            size = src.shape[0] // CHUNKS
            span = pl.ds(step * size, size)
            out.append(pltpu.make_async_copy(src.at[span], dst.at[span], block_sems.at[step, n]))
        return out

    for c in lists:
        c.start()
    for step in range(CHUNKS):
        for c in chunk(step):
            c.start()
    for c in lists:
        c.wait()

    def place(f, slot_axis, per, first_pair, kz):
        dev = f // per
        pos = f % per
        k = (dev % cols) ^ col
        if kz:
            first_pair = first_pair + ((dev // cols) ^ row) * (per // 2)
        block = (k % 2) * (cols // 2) + k // 2
        spot = (block * pairs + first_pair) * 2 + pos
        slot = lax.broadcasted_iota(jnp.int32, f.shape, slot_axis)
        spot = spot ^ (slot % 2)
        return jnp.where(f >= 0, spot, cols * pairs * 2)

    i0_ref[...] = place(f0_ref[...], 0, n0, 0, False)
    i1_ref[...] = place(f1_ref[...], 0, n0 // 2, n0 // 2, False)
    i2_ref[...] = place(f2_ref[...], 1, n0 // 4, n0 // 2 + n0 // 4, False)
    i3_ref[...] = place(f3_ref[...], 1, n0 // 8, n0 // 2 + n0 // 4 + n0 // 8, True)

    @pl.loop(0, CHUNKS)
    def _(step):
        for c in chunk(step):
            c.wait()
        for s_ref, first in ((s3_ref, 0), (s2_ref, n3), (s1_ref, 3 * n3)):
            count = s_ref.shape[0] // CHUNKS
            for j in range(count):
                side_by_side(s_ref, step * count + j, c_ref, first + step * count + j)


def near_kernel(
    n0, leaf, cols, near_src_hbm, x_hbm, blocks_hbm, s_hbm, after_ref, near_ref, c_ref,
    x_ref, near_src_ref, blocks_ref, s_ref, sems, block_sems,
):
    del after_ref
    small = copies([(near_src_hbm, near_src_ref), (x_hbm, x_ref.at[:, pl.ds(0, n0 * leaf)])], sems)

    streams = ((blocks_hbm, blocks_ref), (s_hbm, s_ref))

    def chunk(step):
        span = pl.ds(step * (n0 // STEPS), n0 // STEPS)
        return copies([(src.at[span], dst.at[span]) for src, dst in streams], block_sems.at[step])

    for c in small:
        c.start()
    for step in range(STEPS):
        for c in chunk(step):
            c.start()
    x_ref[:, n0 * leaf :] = jnp.zeros((x_ref.shape[0], leaf), jnp.bfloat16)
    for c in small:
        c.wait()
    first_leaf = (lax.axis_index("row") * cols + lax.axis_index("col")) * n0

    @pl.loop(0, STEPS)
    def _(step):
        for c in chunk(step):
            c.wait()
        for j in range(n0 // STEPS):
            i = step * (n0 // STEPS) + j
            side_by_side(s_ref, i, c_ref, i)
            acc = None
            for s in range(2):
                at = near_src_ref[s, i] - first_leaf
                at = jnp.where((at >= 0) & (at < n0), at, n0)
                xs = x_ref[:, pl.ds(pl.multiple_of(at * leaf, leaf), leaf)]
                part = dot(xs, blocks_ref[i, s], NT)
                acc = part if acc is None else acc + part
            near_ref[:, pl.ds(pl.multiple_of(i * leaf, leaf), leaf)] = acc


def join_kernel(parts, core_ref, after_ref, *refs):
    del after_ref
    out_ref = refs[parts]
    size = refs[0].shape[0]
    for j in range(parts):
        out_ref[j * size : (j + 1) * size] = refs[j][...]
    out_ref[parts * size :] = core_ref[...]


def product_kernel(
    n0, leaf, cols, pairs, i0_hbm, i1_hbm, i2_hbm, i3_hbm, near_src_hbm, a_ref, b_ref, c_ref, c0_ref,
    e1_hbm, e2_hbm, e3_hbm, basis_ref, near_in_ref, x_hbm, blocks_hbm, out_hbm, near_ref,
    i0_ref, i1_ref, i2_ref, i3_ref, near_src_ref, table_ref, field_ref, down_ref, e_ref, x_ref, blocks_ref, out_ref,
    list_sems, sems, out_sems,
):
    del near_in_ref
    nrhs = out_ref.shape[0]
    low = low_half((nrhs, 128))
    chips = cols // 2
    width = HALO * leaf // 128
    block = pairs + 2 * width
    side = 2 * HALO * leaf
    n1, n2, n3 = n0 // 2, n0 // 4, n0 // 8
    ends = [pl.ds(0, HALO), pl.ds(n0 - HALO, HALO)]
    lists = copies(
        [
            (i0_hbm, i0_ref), (i1_hbm, i1_ref), (i2_hbm, i2_ref), (i3_hbm, i3_ref), (near_src_hbm, near_src_ref),
        ],
        list_sems,
    )
    fetch = copies(
        [
            (x_hbm.at[:, pl.ds(0, side)], x_ref.at[:, pl.ds(HALO * leaf, side)]),
            (x_hbm.at[:, pl.ds(n0 * leaf - side, side)], x_ref.at[:, pl.ds(HALO * leaf + side, side)]),
            (blocks_hbm.at[ends[0]], blocks_ref.at[pl.ds(0, HALO)]),
            (blocks_hbm.at[ends[1]], blocks_ref.at[pl.ds(HALO, HALO)]),
            (e3_hbm, e_ref.at[pl.ds(0, n3)]),
            (e2_hbm, e_ref.at[pl.ds(n3, n2)]),
            (e1_hbm, e_ref.at[pl.ds(n3 + n2, n1)]),
        ],
        sems,
    )
    for f in lists + fetch:
        f.start()

    parts = 1
    wide = pairs // parts

    @pl.loop(0, chips * parts)
    def _(t):
        chip, part = t // parts, t % parts
        for h, ref in enumerate((a_ref, b_ref)):
            for j in range(wide):
                v = ref[chip * block + part * wide + j]
                at = ((h * chips + chip) * pairs + part * wide + j) * 2
                table_ref[at] = v
                table_ref[at + 1] = jnp.concatenate([v[:, 64:], v[:, :64]], axis=1)

    table_ref[2 * cols * pairs] = jnp.zeros((nrhs, 128), jnp.bfloat16)
    table_ref[2 * cols * pairs + 1] = jnp.zeros((nrhs, 128), jnp.bfloat16)
    for f in lists:
        f.wait()

    @pl.loop(0, 1)
    def _(t):
        for per, first, spot in (
            (n3, 0, lambda k, i: i3_ref[i, k]),
            (n2, n3, lambda k, i: i2_ref[i, k]),
            (n1, n3 + n2, lambda k, i: i1_ref[k, i]),
            (n0, n3 + n2 + n1, lambda k, i: i0_ref[k, i]),
        ):
            for j in range(per):
                i = t * per + j
                xs = [
                    jnp.where(low, table_ref[spot(2 * q, i)], table_ref[spot(2 * q + 1, i)])
                    for q in range(SLOTS // 2)
                ]
                blocks = c_ref[first + i] if first < 7 * n3 else c0_ref[i]
                field_ref[first + i] = dot(blocks, jnp.concatenate(xs, axis=1), NT)

    row, col = lax.axis_index("row"), lax.axis_index("col")
    odd = col % 2
    across = col + 2 * odd - 1
    inside = (across >= 0) & (across < cols)
    chip = jnp.where(inside, (col ^ across) // 2, chips - 1)
    at_edge = chip * block + pairs + jnp.where(inside, 0, width)
    at_core = chips * block
    left = jnp.where(odd == 1, at_core, at_edge)
    right = jnp.where(odd == 1, at_edge, at_core)
    end = HALO * leaf + 2 * side
    for j in range(width):
        x_ref[:, j * 128 : (j + 1) * 128] = b_ref[left + j]
        x_ref[:, end + j * 128 : end + (j + 1) * 128] = b_ref[right + j]
    zero = 6 * HALO
    x_ref[:, zero * leaf :] = jnp.zeros((nrhs, leaf), jnp.bfloat16)
    for f in fetch:
        f.wait()
    first_leaf = (row * cols + col) * n0

    for j in range(HALO):
        for b, i, shift in ((j, j, HALO), (HALO + j, n0 - HALO + j, 5 * HALO - n0)):
            acc = None
            for s in range(2):
                src = near_src_ref[s, i]
                at = jnp.where(src >= 0, src - first_leaf + shift, zero)
                xs = x_ref[:, pl.ds(pl.multiple_of(at * leaf, leaf), leaf)]
                part = dot(xs, blocks_ref[b, s], NT)
                acc = part if acc is None else acc + part
            near_ref[:, pl.ds(pl.multiple_of(i * leaf, leaf), leaf)] = acc

    down = [field_ref[p].astype(jnp.bfloat16) for p in range(n3)]
    for p in range(7 * n3):
        pair = dot(e_ref[p], down[p], NN)
        for h in range(2):
            c = n3 + 2 * p + h
            down.append((field_ref[c] + pair[h * 64 : (h + 1) * 64]).astype(jnp.bfloat16))
    for i in range(n0):
        down_ref[i] = down[7 * n3 + i]

    def send(t):
        span = pl.ds(pl.multiple_of(t * n0 // SENDS * leaf, leaf), n0 // SENDS * leaf)
        return pltpu.make_async_copy(out_ref.at[:, span], out_hbm.at[:, span], out_sems.at[t])

    @pl.loop(0, SENDS)
    def _(t):
        for j in range(n0 // SENDS):
            i = t * (n0 // SENDS) + j
            d = down_ref[i]
            far = dot(d, basis_ref[t * (n1 // SENDS) + j // 2, (j % 2) * 64 : (j % 2 + 1) * 64], TN)
            at = pl.ds(pl.multiple_of(i * leaf, leaf), leaf)
            out_ref[:, at] = (far + near_ref[:, at]).astype(jnp.bfloat16)
        send(t).start()

    for t in range(SENDS):
        send(t).wait()


def shards(
    points_rhs, leaf_basis, near_src, near_blocks, transfer_first, transfer_second, transfer_third,
    far_zero, far_one, far_two, far_three, couple_zero, couple_one, couple_two, couple_three,
):
    bf, f32, i32 = jnp.bfloat16, jnp.float32, jnp.int32
    n0, leaf, rank = leaf_basis.shape
    nrhs = points_rhs.shape[1]
    rows, cols = lax.axis_size("row"), lax.axis_size("col")
    n1, n2, n3 = n0 // 2, n0 // 4, n0 // 8
    x = points_rhs.T
    basis = leaf_basis.transpose(0, 2, 1).reshape(n1, 2 * rank, leaf)
    e1, e2, e3 = (
        e.reshape(e.shape[0] // 2, 2 * rank, rank) for e in (transfer_first, transfer_second, transfer_third)
    )
    own_pairs = (n0 + n1 + n2) // 2
    top_pairs = n3 // 2
    width = HALO * leaf // 128
    pairs = own_pairs + rows * top_pairs

    def blocks_of(n):
        return jax.ShapeDtypeStruct((n, nrhs, 2 * rank), bf)

    def params(mib):
        return pltpu.CompilerParams(vmem_limit_bytes=mib << 20)

    def cost(us):
        return pl.CostEstimate(flops=int(us * 2e8), bytes_accessed=int(us * 3e6), transcendentals=0)

    skel, near_row, far_row, chip, core = pl.pallas_call(
        functools.partial(upward_kernel, n0, leaf),
        out_shape=[blocks_of(own_pairs), blocks_of(top_pairs + width), blocks_of(top_pairs + width)]
        + [blocks_of(width)] * 2,
        in_specs=[HBM] * 5,
        out_specs=[VMEM] * 5,
        scratch_shapes=[pltpu.VMEM(v.shape, bf) for v in (x, basis, e1, e2, e3)]
        + [pltpu.SemaphoreType.DMA((4,)), pltpu.SemaphoreType.DMA((CHUNKS,))],
        compiler_params=params(12),
        cost_estimate=cost(2),
        name="upward",
    )(*map(in_hbm, (x, basis, e1, e2, e3)))

    def swap(v, axis, size, k):
        return lax.ppermute(v, axis, [(i, i ^ k) for i in range(size)])

    tops = [None] * rows
    for k in reversed(range(1, rows)):
        mersenne = (k & (k + 1)) == 0
        sent = near_row if k == 1 else far_row if mersenne else near_row[:top_pairs]
        tops[k] = swap(sent, "row", rows, k)

    lists = (far_zero.T, far_one.T, far_two, far_three)
    blocks = (couple_one, couple_two, couple_three)
    i0, i1, i2, i3, c = pl.pallas_call(
        functools.partial(fold_kernel, n0, cols, rows),
        out_shape=[jax.ShapeDtypeStruct(f.shape, i32) for f in lists]
        + [jax.ShapeDtypeStruct((7 * n3, rank, SLOTS * rank), bf)],
        in_specs=[HBM] * 7,
        out_specs=[VMEM] * 5,
        scratch_shapes=[pltpu.VMEM(f.shape, i32) for f in lists]
        + [pltpu.VMEM(s.shape, bf) for s in blocks]
        + [pltpu.SemaphoreType.DMA((4,)), pltpu.SemaphoreType.DMA((CHUNKS, 3))],
        compiler_params=params(14),
        cost_estimate=cost(4),
        name="fold",
    )(*map(in_hbm, (*lists, *blocks)))

    mine = pl.pallas_call(
        functools.partial(pack_kernel, rows, cols, top_pairs),
        out_shape=blocks_of(pairs + 2 * width),
        in_specs=[VMEM, VMEM, ANY] + [VMEM] * rows,
        out_specs=VMEM,
        compiler_params=params(4),
        name="pack",
    )(skel, chip, i3, near_row, *reversed(tops[1:]))

    parts = [None] * (cols // 2)
    parts[0] = mine
    for k in reversed(range(1, cols // 2)):
        parts[k] = swap(mine, "col", cols, 2 * k)

    near, c0 = pl.pallas_call(
        functools.partial(near_kernel, n0, leaf, cols),
        out_shape=[
            jax.ShapeDtypeStruct((nrhs, n0 * leaf), f32),
            jax.ShapeDtypeStruct((n0, rank, SLOTS * rank), bf),
        ],
        in_specs=[HBM] * 4 + [ANY],
        out_specs=[VMEM] * 2,
        scratch_shapes=[
            pltpu.VMEM((nrhs, (n0 + 1) * leaf), bf),
            pltpu.SMEM((2, n0), i32),
            pltpu.VMEM(near_blocks.shape, bf),
            pltpu.VMEM(couple_zero.shape, bf),
            pltpu.SemaphoreType.DMA((2,)),
            pltpu.SemaphoreType.DMA((STEPS, 2)),
        ],
        compiler_params=params(18),
        cost_estimate=cost(6),
        name="near",
    )(*map(in_hbm, (near_src.T, x, near_blocks, couple_zero)), mine)

    ours = pl.pallas_call(
        functools.partial(join_kernel, cols // 2),
        out_shape=blocks_of(cols // 2 * mine.shape[0] + width),
        in_specs=[VMEM, ANY] + [VMEM] * (cols // 2),
        out_specs=VMEM,
        compiler_params=params(8),
        name="join",
    )(core, near, *parts)
    theirs = swap(ours, "col", cols, 1)

    out, _ = pl.pallas_call(
        functools.partial(product_kernel, n0, leaf, cols, pairs),
        out_shape=[jax.ShapeDtypeStruct((nrhs, n0 * leaf), bf), jax.ShapeDtypeStruct((nrhs, n0 * leaf), f32)],
        in_specs=[ANY] * 4 + [HBM] + [VMEM] * 4 + [HBM] * 3 + [VMEM] * 2 + [HBM] * 2,
        out_specs=[HBM, VMEM],
        input_output_aliases={13: 1},
        scratch_shapes=[pltpu.SMEM(v.shape, i32) for v in (i0, i1, i2, i3, near_src.T)]
        + [
            pltpu.VMEM((2 * cols * pairs + 2, nrhs, 2 * rank), bf),
            pltpu.VMEM((15 * n3, rank, nrhs), f32),
            pltpu.VMEM((n0, rank, nrhs), bf),
            pltpu.VMEM((7 * n3, 2 * rank, rank), bf),
            pltpu.VMEM((nrhs, (6 * HALO + 1) * leaf), bf),
            pltpu.VMEM((2 * HALO, *near_blocks.shape[1:]), bf),
            pltpu.VMEM((nrhs, n0 * leaf), bf),
            pltpu.SemaphoreType.DMA((5,)),
            pltpu.SemaphoreType.DMA((7,)),
            pltpu.SemaphoreType.DMA((SENDS,)),
        ],
        compiler_params=params(28),
        cost_estimate=cost(5),
        name="product",
    )(
        i0, i1, i2, i3, in_hbm(near_src.T), ours, theirs, c, c0, *map(in_hbm, (e1, e2, e3)), basis, near,
        *map(in_hbm, (x, near_blocks)),
    )
    return out.T


def solution(mesh):
    whole = P(("row", "col"))
    return jax.shard_map(
        shards,
        mesh=mesh,
        in_specs=(whole,) * 15,
        out_specs=whole,
        check_vma=False,
    )
```
